32 devices in a mesh: dp: 1 (over z), tp: 32 (over y, x, core).
Axes of the slice: x: 4, y: 4, z: 1, core: 2. Of those that a mesh axis runs over, the one named last changes fastest.
The devices are a block of a 4x4x8 slice.
Arguments:
- x: bfloat16 [8192, 2048], P(('dp', 'tp'))
- dy: bfloat16 [8192, 2048], P(('dp', 'tp'))
- wg: bfloat16 [2048, 8192], P(None, 'tp')
- wu: bfloat16 [2048, 8192], P(None, 'tp')
- wd: bfloat16 [8192, 2048], P('tp')
- ug: bfloat16 [8192, 8192], P('dp', 'tp')
- uu: bfloat16 [8192, 8192], P('dp', 'tp')
Outputs:
- output 1: bfloat16 [8192, 2048], P(('dp', 'tp'))
- output 2: float32 [2048, 8192], P('dp', 'tp')
- output 3: float32 [2048, 8192], P('dp', 'tp')
- output 4: float32 [8192, 2048], P(('dp', 'tp'))
All inputs are finite; a program needn't handle non-finite values.
Results may differ from the reference program's by a relative error of at most 0.0143732.
Values are sent between devices in bfloat16 or wider.
A program may use at most 768 MiB of HBM per device.

```python
import jax
import jax.numpy as jnp

T = 8192
H = 2048
F = 8192


def setup_inputs(seed: int = 0, part: int = 0) -> dict:
    key = jax.random.key(seed)
    k_shared, k_part = jax.random.split(key)
    kg, ku, kd = jax.random.split(k_shared, 3)
    kx, kdy, kug, kuu = jax.random.split(jax.random.fold_in(k_part, part), 4)
    wg = (jax.random.normal(kg, (H, F), jnp.float32) * H ** -0.5).astype(jnp.bfloat16)
    wu = (jax.random.normal(ku, (H, F), jnp.float32) * H ** -0.5).astype(jnp.bfloat16)
    wd = (jax.random.normal(kd, (F, H), jnp.float32) * F ** -0.5).astype(jnp.bfloat16)
    x = jax.random.normal(kx, (T, H), jnp.float32).astype(jnp.bfloat16)
    dy = jax.random.normal(kdy, (T, H), jnp.float32).astype(jnp.bfloat16)
    ug = jax.random.normal(kug, (T, F), jnp.float32).astype(jnp.bfloat16)
    uu = jax.random.normal(kuu, (T, F), jnp.float32).astype(jnp.bfloat16)
    return {"x": x, "dy": dy, "wg": wg, "wu": wu, "wd": wd, "ug": ug, "uu": uu}


def reference(x, dy, wg, wu, wd, ug, uu):
    ug32 = ug.astype(jnp.float32)
    uu32 = uu.astype(jnp.float32)
    s = jax.nn.sigmoid(ug32)
    a = ug32 * s
    z = (a * uu32).astype(jnp.bfloat16)
    dwd = jnp.dot(z.T, dy, preferred_element_type=jnp.float32)
    g = jnp.dot(dy, wd.T, preferred_element_type=jnp.float32)
    duu = (g * a).astype(jnp.bfloat16)
    dug = (g * uu32 * s * (1.0 + ug32 * (1.0 - s))).astype(jnp.bfloat16)
    p = jnp.dot(dug, wg.T, preferred_element_type=jnp.float32) + jnp.dot(duu, wu.T, preferred_element_type=jnp.float32)
    dx = p.astype(jnp.bfloat16)
    dwg = jnp.dot(x.T, dug, preferred_element_type=jnp.float32)
    dwu = jnp.dot(x.T, duu, preferred_element_type=jnp.float32)
    return (dx, dwg, dwu, dwd)
```

```python
import functools
import math

import jax
import jax.numpy as jnp
from jax import lax
from jax.experimental import pallas as pl
from jax.experimental.pallas import tpu as pltpu
from jax.sharding import PartitionSpec as P

F32 = jnp.float32
BF16 = jnp.bfloat16
S = 4
NR = 4
MESH = pl.DeviceIdType.MESH


def dot(a, b, ca, cb):
    return lax.dot_general(a, b, (((ca,), (cb,)), ((), ())), preferred_element_type=F32)


def kernel(
    n, side,
    x_h, dy_h, wg_h, wu_h, wd_h, ug_h, uu_h,
    dx_h, dwg_h, dwu_h, dwd_h,
    dyb, xb, rsb, rso, pbuf, wdb, wgu, ub, gbuf, dub, zb, accd, accw, recd, recw,
    dy_ss, dy_rs, x_ss, x_rs, rs_ss, rs_rs, u_ss, u_rs, u_ls, w_ss, w_rs, w_ls, own_ls,
    e_ss, e_rs, o_ls,
):
    tb, h = x_h.shape
    fb = wg_h.shape[1]
    rr = tb // NR
    me = lax.axis_index("tp")
    chip = me // 2
    core = lax.rem(me, 2)
    p = chip // side
    q = lax.rem(chip, side)
    pos1 = side * p + lax.rem(q + p, side)
    pos2 = side * q + lax.rem(p + q, side)

    def chip_at(cycle, i):
        a = i // side
        b = lax.rem(lax.rem(i, side) + side - a, side)
        return a * side + b if cycle == 0 else b * side + a

    def ring_chip(r, back):
        here = pos1 if r < 2 else pos2
        d = back if r % 2 == 0 else -back
        return chip_at(r // 2, lax.rem(here - d + 2 * n, n))

    down = [ring_chip(r, -1) * 2 + core for r in range(NR)]
    sib = chip * 2 + 1 - core

    def remote(src, dst, ss, rs, dev):
        return pltpu.make_async_remote_copy(
            src_ref=src, dst_ref=dst, send_sem=ss, recv_sem=rs, device_id={"tp": dev}, device_id_type=MESH
        )

    def hop(buf, ss, rs, s, r):
        a, b = lax.rem(s, S), lax.rem(s + 1, S)
        return remote(buf.at[a, r], buf.at[b, r], ss.at[a, r], rs.at[b, r], down[r])

    def dy_hop(s, r):
        return hop(dyb, dy_ss, dy_rs, s, r)

    def x_hop(s, r):
        return hop(xb, x_ss, x_rs, s, r)

    def rs_hop(s, r):
        a, b = lax.rem(s, 2), lax.rem(s + 1, S)
        return remote(rso.at[a, r], rsb.at[b, r], rs_ss.at[a, r], rs_rs.at[b, r], down[r])

    def u_start(s):
        for r in range(NR):
            o = ring_chip(r, s)
            mine = pl.multiple_of((2 * o + core) * tb + r * rr, rr)
            theirs = pl.multiple_of((2 * o + 1 - core) * tb + r * rr, rr)
            for j, u in enumerate((ug_h, uu_h)):
                pltpu.make_async_copy(u.at[pl.ds(mine, rr)], ub.at[s, 0, j, r], u_ls.at[s]).start()
                remote(u.at[pl.ds(theirs, rr)], ub.at[s, 1, j, r], u_ss.at[s], u_rs.at[s], sib).start()

    weights = ((wd_h, (wdb.at[pl.ds(0, fb)], wdb.at[pl.ds(fb, fb)])),
               (wg_h, (wgu.at[:, pl.ds(0, fb)], wgu.at[:, pl.ds(fb, fb)])),
               (wu_h, (wgu.at[:, pl.ds(2 * fb, fb)], wgu.at[:, pl.ds(3 * fb, fb)])))

    def w_local(i):
        return pltpu.make_async_copy(weights[i][0], weights[i][1][0], w_ls.at[i])

    def w_remote(i):
        return remote(weights[i][0], weights[i][1][1], w_ss.at[i], w_rs.at[i], sib)

    def own(i, r):
        src, dst = ((dy_h, dyb), (x_h, xb))[i]
        return pltpu.make_async_copy(src.at[pl.ds(r * rr, rr)], dst.at[0, r], own_ls.at[i, r])

    barrier = pltpu.get_barrier_semaphore()
    for dev in down + [sib]:
        pl.semaphore_signal(barrier, inc=1, device_id={"tp": dev}, device_id_type=MESH)
    for i in range(2):
        for r in range(NR):
            own(i, r).start()
    for i in range(3):
        w_local(i).start()
    pl.semaphore_wait(barrier, NR + 1)
    for r in range(NR):
        own(0, r).wait()
        dy_hop(0, r).start()
    for i in range(3):
        w_remote(i).start()
    for r in range(NR):
        own(1, r).wait()
        x_hop(0, r).start()
    u_start(0)
    u_start(1)

    def zero(i, _):
        accd[pl.ds(pl.multiple_of(i * (2 * fb // 8), 2 * fb // 8), 2 * fb // 8), :] = jnp.zeros((2 * fb // 8, h), F32)
        accw[pl.ds(pl.multiple_of(i * (h // 8), h // 8), h // 8), :] = jnp.zeros((h // 8, 4 * fb), F32)
        return 0

    lax.fori_loop(0, 8, zero, 0)
    for r in range(NR):
        rsb[1, r] = jnp.zeros((rr, h), BF16)

    ct = min(512, h)
    ht = min(256, h)

    def step(s, _):
        slot = lax.rem(s, S)

        @pl.when(s >= 1)
        def _():
            for r in range(NR):
                dy_hop(s - 1, r).wait_recv()

        @pl.when((s >= 2) & (s < n - 1))
        def _():
            for r in range(NR):
                dy_hop(s - 2, r).wait_send()

        @pl.when((s >= 1) & (s < n - 1))
        def _():
            for r in range(NR):
                dy_hop(s, r).start()

        @pl.when(s + 2 < n)
        def _():
            u_start(s + 2)

        pltpu.make_async_copy(ub.at[s, 0], ub.at[s, 0], u_ls.at[s]).wait()
        u_all = remote(ub.at[s, 1], ub.at[s, 1], u_ss.at[s], u_rs.at[s], sib)
        u_all.wait_recv()

        @pl.when(s == 0)
        def _():
            for i in range(3):
                w_local(i).wait()
                w_remote(i).wait_recv()

        for f in range(2):
            g = dot(dyb[slot].reshape(tb, h), wdb[f * fb:(f + 1) * fb, :], 1, 1)
            gbuf[:, f * fb:(f + 1) * fb] = g
        for f in range(2):
            def act(r, _, f=f):
                rows = pl.ds(pl.multiple_of(r * rr, rr), rr)
                g = gbuf[rows, f * fb:(f + 1) * fb]
                ug = ub[s, f, 0, r].astype(F32)
                uu = ub[s, f, 1, r].astype(F32)
                sg = jax.nn.sigmoid(ug)
                a = ug * sg
                zb[rows, f * fb:(f + 1) * fb] = (a * uu).astype(BF16)
                dub[rows, f * fb:(f + 1) * fb] = (g * uu * sg * (1.0 + ug * (1.0 - sg))).astype(BF16)
                dub[rows, (2 + f) * fb:(3 + f) * fb] = (g * a).astype(BF16)
                return 0

            lax.fori_loop(0, NR, act, 0)

        pi = jnp.where(s == 0, 1, 0)

        def dx_tile(j, _):
            cols = pl.ds(pl.multiple_of(j * ct, ct), ct)
            pbuf[pi, :, cols] = dot(dub[...], wgu[cols, :], 1, 1)
            return 0

        lax.fori_loop(0, h // ct, dx_tile, 0)

        @pl.when(s >= 1)
        def _():
            for r in range(NR):
                x_hop(s - 1, r).wait_recv()

        @pl.when((s >= 2) & (s < n - 1))
        def _():
            for r in range(NR):
                x_hop(s - 2, r).wait_send()

        @pl.when((s >= 1) & (s < n - 1))
        def _():
            for r in range(NR):
                x_hop(s, r).start()

        def dwd_tile(j, _):
            cols = pl.ds(pl.multiple_of(j * ct, ct), ct)
            accd[:, cols] += dot(zb[...], dyb[slot, :, :, cols].reshape(tb, ct), 0, 0)
            return 0

        lax.fori_loop(0, h // ct, dwd_tile, 0)

        @pl.when(s >= 2)
        def _():
            for r in range(NR):
                rs_hop(s - 1, r).wait_recv()

        @pl.when(s >= 3)
        def _():
            for r in range(NR):
                rs_hop(s - 2, r).wait_send()

        @pl.when(s >= 1)
        def _():
            def add(r, _):
                part = pbuf[0, pl.ds(pl.multiple_of(r * rr, rr), rr), :]
                rso[lax.rem(s, 2), r] = (part + rsb[slot, r].astype(F32)).astype(BF16)
                return 0

            lax.fori_loop(0, NR, add, 0)
            for r in range(NR):
                rs_hop(s, r).start()

        def dw_tile(j, _):
            rows = pl.ds(pl.multiple_of(j * ht, ht), ht)
            accw[rows, :] += dot(xb[slot, :, :, rows].reshape(tb, ht), dub[...], 0, 0)
            return 0

        lax.fori_loop(0, h // ht, dw_tile, 0)
        u_all.wait_send()
        return 0

    lax.fori_loop(0, n, step, 0)

    swaps = (remote(accd.at[pl.ds(fb, fb)], recd, e_ss.at[0], e_rs.at[0], sib),
             remote(accw.at[:, pl.ds(fb, fb)], recw.at[0], e_ss.at[1], e_rs.at[1], sib),
             remote(accw.at[:, pl.ds(3 * fb, fb)], recw.at[1], e_ss.at[2], e_rs.at[2], sib))
    for c in swaps:
        c.start()
    for r in range(NR):
        rs_hop(n - 2, r).wait_send()
    outs = []

    swaps[0].wait_recv()
    accd[0:fb, :] += recd[...]
    outs.append(pltpu.make_async_copy(accd.at[pl.ds(0, fb)], dwd_h, o_ls.at[0]))
    outs[-1].start()
    for i, o in enumerate((dwg_h, dwu_h)):
        swaps[1 + i].wait_recv()

        def fold(j, _, i=i):
            rows = pl.ds(pl.multiple_of(j * ht, ht), ht)
            accw[rows, 2 * i * fb:(2 * i + 1) * fb] += recw[i, rows, :]
            return 0

        lax.fori_loop(0, h // ht, fold, 0)
        outs.append(pltpu.make_async_copy(accw.at[:, pl.ds(2 * i * fb, fb)], o, o_ls.at[1 + i]))
        outs[-1].start()

    for r in range(NR):
        rs_hop(n - 1, r).wait_recv()
        rso[0, r] = (pbuf[1, r * rr:(r + 1) * rr, :] + rsb[n % S, r].astype(F32)).astype(BF16)
        outs.append(pltpu.make_async_copy(rso.at[0, r], dx_h.at[pl.ds(r * rr, rr)], o_ls.at[3 + r]))
        outs[-1].start()

    for c in outs:
        c.wait()
    for c in swaps:
        c.wait_send()
    for i in range(3):
        w_remote(i).wait_send()
    for r in range(NR):
        for s in (n - 3, n - 2):
            dy_hop(s, r).wait_send()
            x_hop(s, r).wait_send()
        rs_hop(n - 1, r).wait_send()


def solution(mesh):
    tok = P(("dp", "tp"), None)
    col = P(None, "tp")
    row = P("tp", None)
    act = P("dp", "tp")
    n = mesh.shape["tp"] // 2
    side = math.isqrt(n)

    def body(x, dy, wg, wu, wd, ug, uu):
        tb, h = x.shape
        fb = wg.shape[1]
        rr = tb // NR
        vm = pltpu.VMEM
        dma = pltpu.SemaphoreType.DMA
        flops = 12 * n * tb * h * 2 * fb
        return pl.pallas_call(
            functools.partial(kernel, n, side),
            out_shape=(
                jax.ShapeDtypeStruct((tb, h), BF16),
                jax.ShapeDtypeStruct((h, fb), F32),
                jax.ShapeDtypeStruct((h, fb), F32),
                jax.ShapeDtypeStruct((fb, h), F32),
            ),
            in_specs=[pl.BlockSpec(memory_space=pl.ANY)] * 7,
            out_specs=[pl.BlockSpec(memory_space=pl.ANY)] * 4,
            scratch_shapes=[
                vm((S, NR, rr, h), BF16),
                vm((S, NR, rr, h), BF16),
                vm((S, NR, rr, h), BF16),
                vm((2, NR, rr, h), BF16),
                vm((2, tb, h), F32),
                vm((2 * fb, h), BF16),
                vm((h, 4 * fb), BF16),
                vm((n, 2, 2, NR, rr, fb), BF16),
                vm((tb, 2 * fb), F32),
                vm((tb, 4 * fb), BF16),
                vm((tb, 2 * fb), BF16),
                vm((2 * fb, h), F32),
                vm((h, 4 * fb), F32),
                vm((fb, h), F32),
                vm((2, h, fb), F32),
                dma((S, NR)), dma((S, NR)), dma((S, NR)), dma((S, NR)), dma((2, NR)), dma((S, NR)),
                dma((n,)), dma((n,)), dma((n,)), dma((3,)), dma((3,)), dma((3,)), dma((2, NR)),
                dma((3,)), dma((3,)), dma((3 + NR,)),
            ],
            compiler_params=pltpu.CompilerParams(
                collective_id=0, has_side_effects=True, vmem_limit_bytes=62 * 1024 * 1024
            ),
            cost_estimate=pl.CostEstimate(flops=flops, bytes_accessed=2 * flops // 1000, transcendentals=0),
        )(x, dy, wg, wu, wd, ug, uu)

    return jax.shard_map(
        body, mesh=mesh, in_specs=(tok, tok, col, col, row, act, act), out_specs=(tok, act, act, tok), check_vma=False
    )
```

```python
import functools
import math

import jax
import jax.numpy as jnp
from jax import lax
from jax.experimental import pallas as pl
from jax.experimental.pallas import tpu as pltpu
from jax.sharding import PartitionSpec as P

F32 = jnp.float32
BF16 = jnp.bfloat16
S = 4
MESH = pl.DeviceIdType.MESH


def dot(a, b, ca, cb):
    return lax.dot_general(a, b, (((ca,), (cb,)), ((), ())), preferred_element_type=F32)


def kernel(
    side,
    x_h, dy_h, wg_h, wu_h, wd_h, ug_h, uu_h,
    dx_h, own_d, own_g, own_u, rec_d, rec_g, rec_u, dyl, xl,
    dyt, xt, uo, ux, wdb, wgu, gbuf, zb, dub, accd, accw, pbuf, sin, sout, rsb, rso,
    dyr_s, dyr_r, dyc_s, dyc_r, xr_s, xr_r, xc_s, xc_r, dyt_l, xt_l, u_s, u_r, u_l,
    w_s, w_r, w_l, p_s, p_r, rs_s, rs_r, e_s, e_r, o_l,
):
    _, hb, h = dy_h.shape
    tb = 2 * hb
    q4 = hb // 2
    fb = wg_h.shape[1]
    fh = fb // 2
    m = 2 * side
    me = lax.axis_index("tp")
    chip = me // 2
    core = lax.rem(me, 2)
    other = 1 - core
    py = chip // side
    px = lax.rem(chip, side)
    cls = lax.rem(px + py, side)
    grp = cls // 2
    odd = lax.rem(cls, 2)

    def ring_pos(y, odd_):
        return 2 * lax.rem(side - y, side) + odd_

    def chip_at(g, i):
        k = i // 2
        return lax.rem(side - k, side) * side + lax.rem(k + lax.rem(i, 2) + 2 * g, side)

    def origin(g, pos, d, t):
        return chip_at(g, lax.rem(pos + (2 * m - t if d == 0 else t), m))

    pos = ring_pos(py, odd)
    down = [chip_at(grp, lax.rem(pos + 1, m)) * 2 + core, chip_at(grp, lax.rem(pos + m - 1, m)) * 2 + core]
    sib = chip * 2 + other
    step_ = side - 1 + 2 * odd
    mates = []
    for y, x in ((py, lax.rem(px + step_, side)), (lax.rem(py + step_, side), px)):
        c = lax.rem(x + y, side)
        mates.append(((y * side + x) * 2 + core, c // 2, ring_pos(y, lax.rem(c, 2))))

    def remote(src, dst, ss, rs, dev):
        return pltpu.make_async_remote_copy(
            src_ref=src, dst_ref=dst, send_sem=ss, recv_sem=rs, device_id={"tp": dev}, device_id_type=MESH
        )

    rows = ((dy_h, dyl, dyr_s, dyr_r, dyc_s, dyc_r, dyt, dyt_l), (x_h, xl, xr_s, xr_r, xc_s, xc_r, xt, xt_l))

    def ring(i, s, d, first=False):
        src, land, ss, rs = rows[i][:4]
        return remote(src.at[d] if first else land.at[s, core, d], land.at[s + 1, core, d], ss.at[s, d], rs.at[s + 1, d], down[d])

    def cross(i, s, d, first=False):
        src, land, ss, rs = rows[i][0], rows[i][1], rows[i][4], rows[i][5]
        return remote(src.at[d] if first else land.at[s, core, d], land.at[s, core, d], ss.at[s, d], rs.at[s, d], sib)

    def cross_in(i, s, d):
        land, ss, rs = rows[i][1], rows[i][4], rows[i][5]
        return remote(land.at[s, other, d], land.at[s, other, d], ss.at[s, d], rs.at[s, d], sib)

    def tile_wait(i, t):
        tile, sem = rows[i][6], rows[i][7]
        b = lax.rem(t, 2)
        pltpu.make_async_copy(tile.at[b], tile.at[b], sem.at[b]).wait()

    def tile_load(i, t):
        src, land, tile, sem = rows[i][0], rows[i][1], rows[i][6], rows[i][7]
        b = lax.rem(t, 2)
        for d in range(2):
            cross_in(i, t, d).wait_recv()

        @pl.when(t == 0)
        def _():
            pltpu.make_async_copy(src, tile.at[b, core], sem.at[b]).start()
            pltpu.make_async_copy(land.at[t, other], tile.at[b, other], sem.at[b]).start()

        @pl.when(t > 0)
        def _():
            pltpu.make_async_copy(land.at[t], tile.at[b], sem.at[b]).start()

        if i == 0:
            for d in range(2):
                o = origin(grp, pos, d, t)
                for j, u in enumerate((ug_h, uu_h)):
                    pltpu.make_async_copy(u.at[o, :, d], uo.at[b, j, :, d], u_l.at[b]).start()

    def u_send(t, _):
        for k, (dev, g, p) in enumerate(mates):
            for d in range(2):
                o = origin(g, p, d, t)
                for j, u in enumerate((ug_h, uu_h)):
                    remote(u.at[o, :, d, :, pl.ds(k * fh, fh)], ux.at[t, k, j, :, d], u_s.at[t, k], u_r.at[t, k], dev).start()
        return 0

    def u_all(t, k):
        return remote(ux.at[t, k], ux.at[t, k], u_s.at[t, k], u_r.at[t, k], mates[k][0])

    def w_local(i):
        if i == 0:
            return pltpu.make_async_copy(wd_h, wdb.at[pl.ds(0, fb)], w_l.at[i])
        return pltpu.make_async_copy((wg_h, wu_h)[i - 1], wgu.at[:, pl.ds((i - 1) * 2 * fb, fb)], w_l.at[i])

    def w_remote(i, k):
        if i == 0:
            src, dst = wd_h.at[pl.ds(k * fh, fh)], wdb.at[pl.ds(fb + k * fh, fh)]
        else:
            src = (wg_h, wu_h)[i - 1].at[:, pl.ds(k * fh, fh)]
            dst = wgu.at[:, pl.ds((i - 1) * 2 * fb + fb + k * fh, fh)]
        return remote(src, dst, w_s.at[i, k], w_r.at[i, k], mates[k][0])

    def swap(i, k):
        if i == 0:
            src, dst = accd.at[pl.ds(fb + k * fh, fh)], rec_d.at[pl.ds(k * fh, fh)]
        else:
            src = accw.at[:, pl.ds((i - 1) * 2 * fb + fb + k * fh, fh)]
            dst = (rec_g, rec_u)[i - 1].at[:, pl.ds(k * fh, fh)]
        return remote(src, dst, e_s.at[i, k], e_r.at[i, k], mates[k][0])

    def own_out(i):
        if i == 0:
            return pltpu.make_async_copy(accd.at[pl.ds(0, fb)], own_d, o_l.at[0])
        return pltpu.make_async_copy(accw.at[:, pl.ds((i - 1) * 2 * fb, fb)], (own_g, own_u)[i - 1], o_l.at[i])

    def rs_hop(j, d, z):
        a, b = lax.rem(j, 2), lax.rem(j + 1, S)
        return remote(rso.at[a, d, z], rsb.at[b, d, z], rs_s.at[a, d, z], rs_r.at[b, d, z], down[d])

    def part_hop(j):
        b = lax.rem(j, 2)
        return remote(sout.at[b], sin.at[b], p_s.at[b], p_r.at[b], sib)

    barrier = pltpu.get_barrier_semaphore()
    for dev in down + [sib, mates[0][0], mates[1][0]]:
        pl.semaphore_signal(barrier, inc=1, device_id={"tp": dev}, device_id_type=MESH)
    for i in range(3):
        w_local(i).start()
    pl.semaphore_wait(barrier, 5)
    for d in range(2):
        ring(0, 0, d, True).start()
    for k in range(2):
        w_remote(0, k).start()
    for d in range(2):
        ring(1, 0, d, True).start()
    for d in range(2):
        cross(0, 0, d, True).start()
    lax.fori_loop(0, m, u_send, 0)
    for d in range(2):
        cross(1, 0, d, True).start()
    for i in (1, 2):
        for k in range(2):
            w_remote(i, k).start()

    def zero(i, _):
        accd[pl.ds(pl.multiple_of(i * (2 * fb // 8), 2 * fb // 8), 2 * fb // 8), :] = jnp.zeros((2 * fb // 8, h), F32)
        accw[pl.ds(pl.multiple_of(i * (h // 8), h // 8), h // 8), :] = jnp.zeros((h // 8, 4 * fb), F32)
        return 0

    lax.fori_loop(0, 8, zero, 0)

    ct = min(512, h)
    ht = min(256, h)

    def forward(i, v):
        @pl.when((v >= 1) & (v < m))
        def _():
            for d in range(2):
                ring(i, v - 1, d).wait_recv()

                @pl.when(v < m - 1)
                def _(d=d):
                    ring(i, v, d).start()

                cross(i, v, d).start()

    def count(v):
        return jnp.maximum(jnp.minimum(v + jnp.where(v >= 3, 1, 0), m), 0)

    def grads(t, hi):
        b = lax.rem(t, 2)

        @pl.when(t + 1 < hi)
        def _():
            tile_load(0, t + 1)

        @pl.when(t == 0)
        def _():
            w_local(0).wait()
            for k in range(2):
                w_remote(0, k).wait_recv()

        for k in range(2):
            u_all(t, k).wait_recv()
        pltpu.make_async_copy(uo.at[b], uo.at[b], u_l.at[b]).wait()
        tile_wait(0, t)
        for f in range(2):
            gbuf[:, f * fb:(f + 1) * fb] = dot(dyt[b].reshape(2 * tb, h), wdb[f * fb:(f + 1) * fb, :], 1, 1)

        def act(r, _):
            c, d = r // 2, lax.rem(r, 2)
            rws = pl.ds(pl.multiple_of(r * hb, hb), hb)
            half = pl.ds(pl.multiple_of(d * hb, hb), hb)
            for lo, n, get in (
                (0, fb, lambda j: uo[b, j, c, d]),
                (fb, fh, lambda j: ux[t, 0, j, c, d]),
                (fb + fh, fh, lambda j: ux[t, 1, j, c, d]),
            ):
                g = gbuf[rws, lo:lo + n]
                ug = get(0).astype(F32)
                uu = get(1).astype(F32)
                sg = jax.nn.sigmoid(ug)
                a = ug * sg
                zb[rws, lo:lo + n] = (a * uu).astype(BF16)
                dub[t, c, half, lo:lo + n] = (g * uu * sg * (1.0 + ug * (1.0 - sg))).astype(BF16)
                dub[t, c, half, 2 * fb + lo:2 * fb + lo + n] = (g * a).astype(BF16)
            return 0

        lax.fori_loop(0, 4, act, 0)

        def dwd_tile(j, _):
            cols = pl.ds(pl.multiple_of(j * ct, ct), ct)
            accd[:, cols] += dot(zb[...], dyt[b, :, :, :, cols].reshape(2 * tb, ct), 0, 0)
            return 0

        lax.fori_loop(0, h // ct, dwd_tile, 0)

    def weight_grads(t, hi):
        b = lax.rem(t, 2)

        @pl.when(t + 1 < hi)
        def _():
            tile_load(1, t + 1)

        tile_wait(1, t)

        def dw_tile(j, _):
            cols = pl.ds(pl.multiple_of(j * ht, ht), ht)
            accw[cols, :] += dot(xt[b, :, :, :, cols].reshape(2 * tb, ht), dub[t].reshape(2 * tb, 4 * fb), 0, 0)
            return 0

        lax.fori_loop(0, h // ht, dw_tile, 0)

    def partial(j):
        t = lax.rem(j, m)
        b = lax.rem(j, 2)

        @pl.when(j >= 3)
        def _():
            part_hop(j - 2).wait_send()

        def send_tile(c, _):
            cols = pl.ds(pl.multiple_of(c * ct, ct), ct)
            sout[b, :, cols] = dot(dub[t, other], wgu[cols, :], 1, 1).astype(BF16)
            return 0

        lax.fori_loop(0, h // ct, send_tile, 0)

        def keep_tile(c, _):
            cols = pl.ds(pl.multiple_of(c * ct, ct), ct)
            pbuf[:, cols] = dot(dub[t, core], wgu[cols, :], 1, 1)
            return 0

        lax.fori_loop(0, h // ct, keep_tile, 0)
        part_hop(j).start()

    def total(j, d, z, first):
        lo = pl.multiple_of(d * hb + z * q4, q4)
        v = pbuf[pl.ds(lo, q4), :] + sin[lax.rem(j, 2), pl.ds(lo, q4), :].astype(F32)
        if not first:
            v = v + rsb[lax.rem(j, S), d, z].astype(F32)
        return v.astype(BF16)

    def step(v, _):
        a0, a1 = count(v - 1), count(v)
        c0, c1 = count(v - 2), a0
        forward(0, v)

        @pl.when(a0 < a1)
        def _():
            tile_load(0, a0)

        def c_body(t, _):
            weight_grads(t, c1)
            return 0

        lax.fori_loop(c0, c1, c_body, 0)
        forward(1, v)

        @pl.when(a0 < a1)
        def _():
            tile_load(1, a0)

        def a_body(t, _):
            grads(t, a1)
            return 0

        lax.fori_loop(a0, a1, a_body, 0)

        @pl.when(v == m - 1)
        def _():
            for k in range(2):
                swap(0, k).start()
            own_out(0).start()

        @pl.when(v == m)
        def _():
            for i in (1, 2):
                for k in range(2):
                    swap(i, k).start()
                own_out(i).start()

        j = v - (m - 3)

        @pl.when(j >= 1)
        def _():
            part_hop(j).wait_recv()

            @pl.when(j >= 3)
            def _():
                for d in range(2):
                    for z in range(2):
                        rs_hop(j - 2, d, z).wait_send()

            for z in range(2):
                @pl.when(j >= 2)
                def _(z=z):
                    for d in range(2):
                        rs_hop(j - 1, d, z).wait_recv()
                        rso[lax.rem(j, 2), d, z] = total(j, d, z, False)

                @pl.when(j == 1)
                def _(z=z):
                    for d in range(2):
                        rso[lax.rem(j, 2), d, z] = total(j, d, z, True)

                for d in range(2):
                    rs_hop(j, d, z).start()

        @pl.when(j == 0)
        def _():
            for i in (1, 2):
                w_local(i).wait()
                for k in range(2):
                    w_remote(i, k).wait_recv()

        @pl.when(j >= 0)
        def _():
            partial(j + 1)

        return 0

    lax.fori_loop(0, 2 * m - 3, step, 0)

    part_hop(m).wait_recv()
    outs = []
    for d in range(2):
        for z in range(2):
            rs_hop(m - 2, d, z).wait_send()
    for z in range(2):
        for d in range(2):
            rs_hop(m - 1, d, z).wait_recv()
            rso[m % 2, d, z] = total(m, d, z, False)
            outs.append(pltpu.make_async_copy(rso.at[m % 2, d, z], dx_h.at[pl.ds(d * hb + z * q4, q4)], o_l.at[3 + 2 * d + z]))
            outs[-1].start()

    for i in range(3):
        own_out(i).wait()
        for k in range(2):
            swap(i, k).wait()
            w_remote(i, k).wait_send()
    for j in (m - 1, m):
        part_hop(j).wait_send()
    for d in range(2):
        for z in range(2):
            rs_hop(m - 1, d, z).wait_send()

    def drain(s, _):
        for k in range(2):
            u_all(s, k).wait_send()
        for i in range(2):
            for d in range(2):
                cross(i, s, d).wait_send()

                @pl.when(s < m - 1)
                def _(i=i, d=d):
                    ring(i, s, d).wait_send()
        return 0

    lax.fori_loop(0, m, drain, 0)
    for c in outs:
        c.wait()


def solution(mesh):
    tok = P(("dp", "tp"), None)
    col = P(None, "tp")
    row = P("tp", None)
    act = P("dp", "tp")
    n = mesh.shape["tp"] // 2
    side = math.isqrt(n)
    m = 2 * side

    def body(x, dy, wg, wu, wd, ug, uu):
        tb, h = x.shape
        fb = wg.shape[1]
        hb, fh = tb // 2, fb // 2
        vm = pltpu.VMEM
        dma = pltpu.SemaphoreType.DMA
        sds = jax.ShapeDtypeStruct
        flops = 12 * n * tb * h * 2 * fb
        dx, own_d, own_g, own_u, rec_d, rec_g, rec_u, _, _ = pl.pallas_call(
            functools.partial(kernel, side),
            out_shape=(
                sds((tb, h), BF16),
                sds((fb, h), F32), sds((h, fb), F32), sds((h, fb), F32),
                sds((fb, h), F32), sds((h, fb), F32), sds((h, fb), F32),
                sds((m, 2, 2, hb, h), BF16), sds((m, 2, 2, hb, h), BF16),
            ),
            in_specs=[pl.BlockSpec(memory_space=pl.ANY)] * 7,
            out_specs=[pl.BlockSpec(memory_space=pl.ANY)] * 9,
            scratch_shapes=[
                vm((2, 2, 2, hb, h), BF16),
                vm((2, 2, 2, hb, h), BF16),
                vm((2, 2, 2, 2, hb, fb), BF16),
                vm((m, 2, 2, 2, 2, hb, fh), BF16),
                vm((2 * fb, h), BF16),
                vm((h, 4 * fb), BF16),
                vm((2 * tb, 2 * fb), F32),
                vm((2 * tb, 2 * fb), BF16),
                vm((m, 2, tb, 4 * fb), BF16),
                vm((2 * fb, h), F32),
                vm((h, 4 * fb), F32),
                vm((tb, h), F32),
                vm((2, tb, h), BF16),
                vm((2, tb, h), BF16),
                vm((S, 2, 2, hb // 2, h), BF16),
                vm((2, 2, 2, hb // 2, h), BF16),
                dma((m, 2)), dma((m, 2)), dma((m, 2)), dma((m, 2)),
                dma((m, 2)), dma((m, 2)), dma((m, 2)), dma((m, 2)),
                dma((2,)), dma((2,)), dma((m, 2)), dma((m, 2)), dma((2,)),
                dma((3, 2)), dma((3, 2)), dma((3,)), dma((2,)), dma((2,)),
                dma((2, 2, 2)), dma((S, 2, 2)), dma((3, 2)), dma((3, 2)), dma((7,)),
            ],
            compiler_params=pltpu.CompilerParams(
                collective_id=0, has_side_effects=True, vmem_limit_bytes=62 * 1024 * 1024
            ),
            cost_estimate=pl.CostEstimate(flops=flops, bytes_accessed=2 * flops // 1000, transcendentals=0),
        )(
            x.reshape(2, hb, h), dy.reshape(2, hb, h), wg, wu, wd,
            ug.reshape(n, 2, 2, hb, fb), uu.reshape(n, 2, 2, hb, fb),
        )
        return dx, own_g + rec_g, own_u + rec_u, own_d + rec_d

    return jax.shard_map(
        body, mesh=mesh, in_specs=(tok, tok, col, col, row, act, act), out_specs=(tok, act, act, tok), check_vma=False
    )
```

```python
import functools
import math

import jax
import jax.numpy as jnp
from jax import lax
from jax.experimental import pallas as pl
from jax.experimental.pallas import tpu as pltpu
from jax.sharding import PartitionSpec as P

F32 = jnp.float32
BF16 = jnp.bfloat16
S = 4
MESH = pl.DeviceIdType.MESH


def dot(a, b, ca, cb):
    return lax.dot_general(a, b, (((ca,), (cb,)), ((), ())), preferred_element_type=F32)


def kernel(
    side,
    x_h, dy_h, wg_h, wu_h, wd_h, ug_h, uu_h,
    dx_h, own_d, own_g, own_u, rec_d, rec_g, rec_u, dyl, xl, rl,
    dyt, xt, uo, ux, wdb, wgu, gbuf, zb, dub, accd, accw, pbuf, sin, sout, rsb, rso,
    dyr_s, dyr_r, dyc_s, dyc_r, xr_s, xr_r, xc_s, xc_r, dyt_l, xt_l, u_s, u_r, u_l,
    w_s, w_r, w_l, p_s, p_r, rs_s, rs_r, e_s, e_r, o_l, b_s, b_r, l_s,
):
    _, hb, h = dy_h.shape
    tb = 2 * hb
    q4 = hb // 2
    fb = wg_h.shape[1]
    fh = fb // 2
    m = 2 * side
    me = lax.axis_index("tp")
    chip = me // 2
    core = lax.rem(me, 2)
    other = 1 - core
    py = chip // side
    px = lax.rem(chip, side)
    cls = lax.rem(px + py, side)
    grp = cls // 2
    odd = lax.rem(cls, 2)

    def ring_pos(y, odd_):
        return 2 * lax.rem(side - y, side) + odd_

    def chip_at(g, i):
        k = i // 2
        return lax.rem(side - k, side) * side + lax.rem(k + lax.rem(i, 2) + 2 * g, side)

    def origin(g, pos, d, t):
        return chip_at(g, lax.rem(pos + (2 * m - t if d == 0 else t), m))

    pos = ring_pos(py, odd)
    down = [chip_at(grp, lax.rem(pos + 1, m)) * 2 + core, chip_at(grp, lax.rem(pos + m - 1, m)) * 2 + core]
    sib = chip * 2 + other
    step_ = side - 1 + 2 * odd
    mates = []
    for y, x in ((py, lax.rem(px + step_, side)), (lax.rem(py + step_, side), px)):
        c = lax.rem(x + y, side)
        mates.append(((y * side + x) * 2 + core, c // 2, ring_pos(y, lax.rem(c, 2))))

    leave = [jnp.where(odd == d, mates[1][0], mates[0][0]) for d in range(2)]

    def remote(src, dst, ss, rs, dev):
        return pltpu.make_async_remote_copy(
            src_ref=src, dst_ref=dst, send_sem=ss, recv_sem=rs, device_id={"tp": dev}, device_id_type=MESH
        )

    rows = ((dy_h, dyl, dyr_s, dyr_r, dyc_s, dyc_r, dyt, dyt_l), (x_h, xl, xr_s, xr_r, xc_s, xc_r, xt, xt_l))

    def ring(i, s, d, first=False):
        src, land, ss, rs = rows[i][:4]
        return remote(src.at[d] if first else land.at[s, core, d], land.at[s + 1, core, d], ss.at[s, d], rs.at[s + 1, d], down[d])

    def away(k, d, first=False):
        return remote(x_h.at[d] if first else xl.at[2 * k, core, d], rl.at[k, d], b_s.at[k, d], b_r.at[k, d], leave[d])

    def relay(k, d):
        return remote(rl.at[k, d], xl.at[2 * k + 2, core, d], l_s.at[k, d], xr_r.at[2 * k + 2, d], leave[d])

    def cross(i, s, d, first=False):
        src, land, ss, rs = rows[i][0], rows[i][1], rows[i][4], rows[i][5]
        return remote(src.at[d] if first else land.at[s, core, d], land.at[s, core, d], ss.at[s, d], rs.at[s, d], sib)

    def cross_in(i, s, d):
        land, ss, rs = rows[i][1], rows[i][4], rows[i][5]
        return remote(land.at[s, other, d], land.at[s, other, d], ss.at[s, d], rs.at[s, d], sib)

    def tile_wait(i, t):
        tile, sem = rows[i][6], rows[i][7]
        b = lax.rem(t, 2)
        pltpu.make_async_copy(tile.at[b], tile.at[b], sem.at[b]).wait()

    def tile_load(i, t):
        src, land, tile, sem = rows[i][0], rows[i][1], rows[i][6], rows[i][7]
        b = lax.rem(t, 2)
        for d in range(2):
            cross_in(i, t, d).wait_recv()

        @pl.when(t == 0)
        def _():
            pltpu.make_async_copy(src, tile.at[b, core], sem.at[b]).start()
            pltpu.make_async_copy(land.at[t, other], tile.at[b, other], sem.at[b]).start()

        @pl.when(t > 0)
        def _():
            pltpu.make_async_copy(land.at[t], tile.at[b], sem.at[b]).start()

        if i == 0:
            for d in range(2):
                o = origin(grp, pos, d, t)
                for j, u in enumerate((ug_h, uu_h)):
                    pltpu.make_async_copy(u.at[o, :, d], uo.at[b, j, :, d], u_l.at[b]).start()

    def u_send(t, _):
        for k, (dev, g, p) in enumerate(mates):
            for d in range(2):
                o = origin(g, p, d, t)
                for j, u in enumerate((ug_h, uu_h)):
                    remote(u.at[o, :, d, :, pl.ds(k * fh, fh)], ux.at[t, k, j, :, d], u_s.at[t, k], u_r.at[t, k], dev).start()
        return 0

    def u_all(t, k):
        return remote(ux.at[t, k], ux.at[t, k], u_s.at[t, k], u_r.at[t, k], mates[k][0])

    def w_local(i):
        if i == 0:
            return pltpu.make_async_copy(wd_h, wdb.at[pl.ds(0, fb)], w_l.at[i])
        return pltpu.make_async_copy((wg_h, wu_h)[i - 1], wgu.at[:, pl.ds((i - 1) * 2 * fb, fb)], w_l.at[i])

    def w_remote(i, k):
        if i == 0:
            src, dst = wd_h.at[pl.ds(k * fh, fh)], wdb.at[pl.ds(fb + k * fh, fh)]
        else:
            src = (wg_h, wu_h)[i - 1].at[:, pl.ds(k * fh, fh)]
            dst = wgu.at[:, pl.ds((i - 1) * 2 * fb + fb + k * fh, fh)]
        return remote(src, dst, w_s.at[i, k], w_r.at[i, k], mates[k][0])

    def swap(i, k):
        if i == 0:
            src, dst = accd.at[pl.ds(fb + k * fh, fh)], rec_d.at[pl.ds(k * fh, fh)]
        else:
            src = accw.at[:, pl.ds((i - 1) * 2 * fb + fb + k * fh, fh)]
            dst = (rec_g, rec_u)[i - 1].at[:, pl.ds(k * fh, fh)]
        return remote(src, dst, e_s.at[i, k], e_r.at[i, k], mates[k][0])

    def own_out(i):
        if i == 0:
            return pltpu.make_async_copy(accd.at[pl.ds(0, fb)], own_d, o_l.at[0])
        return pltpu.make_async_copy(accw.at[:, pl.ds((i - 1) * 2 * fb, fb)], (own_g, own_u)[i - 1], o_l.at[i])

    def rs_hop(j, d, z):
        a, b = lax.rem(j, 2), lax.rem(j + 1, S)
        return remote(rso.at[a, d, z], rsb.at[b, d, z], rs_s.at[a, d, z], rs_r.at[b, d, z], down[d])

    def part_hop(j):
        b = lax.rem(j, 2)
        return remote(sout.at[b], sin.at[b], p_s.at[b], p_r.at[b], sib)

    barrier = pltpu.get_barrier_semaphore()
    for dev in down + [sib, mates[0][0], mates[1][0]]:
        pl.semaphore_signal(barrier, inc=1, device_id={"tp": dev}, device_id_type=MESH)
    for i in range(3):
        w_local(i).start()
    pl.semaphore_wait(barrier, 5)
    for d in range(2):
        ring(0, 0, d, True).start()
        away(0, d, True).start()
    for k in range(2):
        w_remote(0, k).start()
    for d in range(2):
        ring(1, 0, d, True).start()
    for d in range(2):
        cross(0, 0, d, True).start()
    u_send(0, 0)
    u_send(1, 0)
    for d in range(2):
        cross(1, 0, d, True).start()

    def zero(i, _):
        accd[pl.ds(pl.multiple_of(i * (2 * fb // 8), 2 * fb // 8), 2 * fb // 8), :] = jnp.zeros((2 * fb // 8, h), F32)
        accw[pl.ds(pl.multiple_of(i * (h // 8), h // 8), h // 8), :] = jnp.zeros((h // 8, 4 * fb), F32)
        return 0

    lax.fori_loop(0, 8, zero, 0)

    ct = min(512, h)
    ht = min(256, h)

    def forward_dy(v):
        @pl.when((v >= 1) & (v < m))
        def _():
            for d in range(2):
                ring(0, v - 1, d).wait_recv()

                @pl.when(v < m - 1)
                def _(d=d):
                    ring(0, v, d).start()

                cross(0, v, d).start()

    def forward_x(v):
        k = v // 2

        @pl.when((v >= 1) & (v < m) & (lax.rem(v, 2) == 1))
        def _():
            @pl.when(v < m - 1)
            def _():
                for d in range(2):
                    away(k, d).wait_recv()
                    relay(k, d).start()

            for d in range(2):
                ring(1, v - 1, d).wait_recv()
                cross(1, v, d).start()

        @pl.when((v >= 1) & (v < m) & (lax.rem(v, 2) == 0))
        def _():
            for d in range(2):
                relay(k - 1, d).wait_recv()

                @pl.when(v < m - 2)
                def _(d=d):
                    away(k, d).start()

                ring(1, v, d).start()
                cross(1, v, d).start()

    def count(v):
        return jnp.maximum(jnp.minimum(v + jnp.where(v >= 3, 1, 0), m), 0)

    def grads(t, hi):
        b = lax.rem(t, 2)

        @pl.when(t + 1 < hi)
        def _():
            tile_load(0, t + 1)

        @pl.when(t == 0)
        def _():
            w_local(0).wait()
            for k in range(2):
                w_remote(0, k).wait_recv()

        for k in range(2):
            u_all(t, k).wait_recv()
        pltpu.make_async_copy(uo.at[b], uo.at[b], u_l.at[b]).wait()
        tile_wait(0, t)
        for f in range(2):
            gbuf[:, f * fb:(f + 1) * fb] = dot(dyt[b].reshape(2 * tb, h), wdb[f * fb:(f + 1) * fb, :], 1, 1)

        def act(r, _):
            c, d = r // 2, lax.rem(r, 2)
            rws = pl.ds(pl.multiple_of(r * hb, hb), hb)
            half = pl.ds(pl.multiple_of(d * hb, hb), hb)
            for lo, n, get in (
                (0, fb, lambda j: uo[b, j, c, d]),
                (fb, fh, lambda j: ux[t, 0, j, c, d]),
                (fb + fh, fh, lambda j: ux[t, 1, j, c, d]),
            ):
                g = gbuf[rws, lo:lo + n]
                ug = get(0).astype(F32)
                uu = get(1).astype(F32)
                sg = jax.nn.sigmoid(ug)
                a = ug * sg
                zb[rws, lo:lo + n] = (a * uu).astype(BF16)
                dub[t, c, half, lo:lo + n] = (g * uu * sg * (1.0 + ug * (1.0 - sg))).astype(BF16)
                dub[t, c, half, 2 * fb + lo:2 * fb + lo + n] = (g * a).astype(BF16)
            return 0

        lax.fori_loop(0, 4, act, 0)

        def dwd_tile(j, _):
            cols = pl.ds(pl.multiple_of(j * ct, ct), ct)
            accd[:, cols] += dot(zb[...], dyt[b, :, :, :, cols].reshape(2 * tb, ct), 0, 0)
            return 0

        lax.fori_loop(0, h // ct, dwd_tile, 0)

    def weight_grads(t, hi):
        b = lax.rem(t, 2)

        @pl.when(t + 1 < hi)
        def _():
            tile_load(1, t + 1)

        tile_wait(1, t)

        def dw_tile(j, _):
            cols = pl.ds(pl.multiple_of(j * ht, ht), ht)
            accw[cols, :] += dot(xt[b, :, :, :, cols].reshape(2 * tb, ht), dub[t].reshape(2 * tb, 4 * fb), 0, 0)
            return 0

        lax.fori_loop(0, h // ht, dw_tile, 0)

    def partial(j):
        t = lax.rem(j, m)
        b = lax.rem(j, 2)

        @pl.when(j >= 3)
        def _():
            part_hop(j - 2).wait_send()

        def send_tile(c, _):
            cols = pl.ds(pl.multiple_of(c * ct, ct), ct)
            sout[b, :, cols] = dot(dub[t, other], wgu[cols, :], 1, 1).astype(BF16)
            return 0

        lax.fori_loop(0, h // ct, send_tile, 0)

        def keep_tile(c, _):
            cols = pl.ds(pl.multiple_of(c * ct, ct), ct)
            pbuf[:, cols] = dot(dub[t, core], wgu[cols, :], 1, 1)
            return 0

        lax.fori_loop(0, h // ct, keep_tile, 0)
        part_hop(j).start()

    def total(j, d, z, first):
        lo = pl.multiple_of(d * hb + z * q4, q4)
        v = pbuf[pl.ds(lo, q4), :] + sin[lax.rem(j, 2), pl.ds(lo, q4), :].astype(F32)
        if not first:
            v = v + rsb[lax.rem(j, S), d, z].astype(F32)
        return v.astype(BF16)

    def step(v, _):
        a0, a1 = count(v - 1), count(v)
        c0, c1 = count(v - 2), jnp.minimum(a0, m - 1)
        forward_dy(v)

        @pl.when(a0 < a1)
        def _():
            tile_load(0, a0)

        def c_body(t, _):
            weight_grads(t, c1)
            return 0

        lax.fori_loop(c0, c1, c_body, 0)
        forward_x(v)

        @pl.when(v + 2 < m)
        def _():
            u_send(v + 2, 0)

        for i in (1, 2):
            @pl.when(v == i)
            def _(i=i):
                for k in range(2):
                    w_remote(i, k).start()

        @pl.when(a0 < a1)
        def _():
            tile_load(1, a0)

        def a_body(t, _):
            grads(t, a1)
            return 0

        lax.fori_loop(a0, a1, a_body, 0)

        @pl.when(v == m - 1)
        def _():
            for k in range(2):
                swap(0, k).start()
            own_out(0).start()
            weight_grads(v, m)
            for i in (1, 2):
                for k in range(2):
                    swap(i, k).start()
                own_out(i).start()

        j = v - (m - 4)

        @pl.when(j >= 1)
        def _():
            part_hop(j).wait_recv()

            @pl.when(j >= 3)
            def _():
                for d in range(2):
                    for z in range(2):
                        rs_hop(j - 2, d, z).wait_send()

            for z in range(2):
                @pl.when(j >= 2)
                def _(z=z):
                    for d in range(2):
                        rs_hop(j - 1, d, z).wait_recv()
                        rso[lax.rem(j, 2), d, z] = total(j, d, z, False)

                @pl.when(j == 1)
                def _(z=z):
                    for d in range(2):
                        rso[lax.rem(j, 2), d, z] = total(j, d, z, True)

                for d in range(2):
                    rs_hop(j, d, z).start()

        @pl.when(j == 0)
        def _():
            for i in (1, 2):
                w_local(i).wait()
                for k in range(2):
                    w_remote(i, k).wait_recv()

        @pl.when(j >= 0)
        def _():
            partial(j + 1)

        return 0

    lax.fori_loop(0, 2 * m - 4, step, 0)

    part_hop(m).wait_recv()
    outs = []
    for d in range(2):
        for z in range(2):
            rs_hop(m - 2, d, z).wait_send()
    for z in range(2):
        for d in range(2):
            rs_hop(m - 1, d, z).wait_recv()
            rso[m % 2, d, z] = total(m, d, z, False)
            outs.append(pltpu.make_async_copy(rso.at[m % 2, d, z], dx_h.at[pl.ds(d * hb + z * q4, q4)], o_l.at[3 + 2 * d + z]))
            outs[-1].start()

    for i in range(3):
        own_out(i).wait()
        for k in range(2):
            swap(i, k).wait()
            w_remote(i, k).wait_send()
    for j in (m - 1, m):
        part_hop(j).wait_send()
    for d in range(2):
        for z in range(2):
            rs_hop(m - 1, d, z).wait_send()

    def drain(s, _):
        for k in range(2):
            u_all(s, k).wait_send()
        for i in range(2):
            for d in range(2):
                cross(i, s, d).wait_send()

                @pl.when(s < m - 1 if i == 0 else lax.rem(s, 2) == 0)
                def _(i=i, d=d):
                    ring(i, s, d).wait_send()
        return 0

    lax.fori_loop(0, m, drain, 0)
    for k in range(side - 1):
        for d in range(2):
            away(k, d).wait_send()
            relay(k, d).wait_send()
    for c in outs:
        c.wait()


def solution(mesh):
    tok = P(("dp", "tp"), None)
    col = P(None, "tp")
    row = P("tp", None)
    act = P("dp", "tp")
    n = mesh.shape["tp"] // 2
    side = math.isqrt(n)
    m = 2 * side

    def body(x, dy, wg, wu, wd, ug, uu):
        tb, h = x.shape
        fb = wg.shape[1]
        hb, fh = tb // 2, fb // 2
        vm = pltpu.VMEM
        dma = pltpu.SemaphoreType.DMA
        sds = jax.ShapeDtypeStruct
        flops = 12 * n * tb * h * 2 * fb
        dx, own_d, own_g, own_u, rec_d, rec_g, rec_u, _, _, _ = pl.pallas_call(
            functools.partial(kernel, side),
            out_shape=(
                sds((tb, h), BF16),
                sds((fb, h), F32), sds((h, fb), F32), sds((h, fb), F32),
                sds((fb, h), F32), sds((h, fb), F32), sds((h, fb), F32),
                sds((m, 2, 2, hb, h), BF16), sds((m, 2, 2, hb, h), BF16), sds((side - 1, 2, hb, h), BF16),
            ),
            in_specs=[pl.BlockSpec(memory_space=pltpu.HBM)] * 7,
            out_specs=[pl.BlockSpec(memory_space=pl.ANY)] * 10,
            scratch_shapes=[
                vm((2, 2, 2, hb, h), BF16),
                vm((2, 2, 2, hb, h), BF16),
                vm((2, 2, 2, 2, hb, fb), BF16),
                vm((m, 2, 2, 2, 2, hb, fh), BF16),
                vm((2 * fb, h), BF16),
                vm((h, 4 * fb), BF16),
                vm((2 * tb, 2 * fb), F32),
                vm((2 * tb, 2 * fb), BF16),
                vm((m, 2, tb, 4 * fb), BF16),
                vm((2 * fb, h), F32),
                vm((h, 4 * fb), F32),
                vm((tb, h), F32),
                vm((2, tb, h), BF16),
                vm((2, tb, h), BF16),
                vm((S, 2, 2, hb // 2, h), BF16),
                vm((2, 2, 2, hb // 2, h), BF16),
                dma((m, 2)), dma((m, 2)), dma((m, 2)), dma((m, 2)),
                dma((m, 2)), dma((m, 2)), dma((m, 2)), dma((m, 2)),
                dma((2,)), dma((2,)), dma((m, 2)), dma((m, 2)), dma((2,)),
                dma((3, 2)), dma((3, 2)), dma((3,)), dma((2,)), dma((2,)),
                dma((2, 2, 2)), dma((S, 2, 2)), dma((3, 2)), dma((3, 2)), dma((7,)),
                dma((side - 1, 2)), dma((side - 1, 2)), dma((side - 1, 2)),
            ],
            compiler_params=pltpu.CompilerParams(
                collective_id=0, has_side_effects=True, vmem_limit_bytes=62 * 1024 * 1024
            ),
            cost_estimate=pl.CostEstimate(flops=flops, bytes_accessed=2 * flops // 1000, transcendentals=0),
        )(
            x.reshape(2, hb, h), dy.reshape(2, hb, h), wg, wu, wd,
            ug.reshape(n, 2, 2, hb, fb), uu.reshape(n, 2, 2, hb, fb),
        )
        return dx, own_g + rec_g, own_u + rec_u, own_d + rec_d

    return jax.shard_map(
        body, mesh=mesh, in_specs=(tok, tok, col, col, row, act, act), out_specs=(tok, act, act, tok), check_vma=False
    )
```

```python
import functools
import math

import jax
import jax.numpy as jnp
from jax import lax
from jax.experimental import pallas as pl
from jax.experimental.pallas import tpu as pltpu
from jax.sharding import PartitionSpec as P

F32 = jnp.float32
BF16 = jnp.bfloat16
S = 4
MESH = pl.DeviceIdType.MESH
PLAN = (
    "W0", "a0", "c0", "U0", "Y1", "L0", "a1", "O1", "c1", "U1", "A0", "C0", "U2", "Y2", "U3", "a2", "E2",
    "c2", "A1", "C1", "Y3", "A2", "W1", "a3", "C2", "A3", "O3", "W2", "L1", "c3", "C3", "Y4", "a4", "Y5",
    "U4", "P1", "a5", "P2", "U5", "R2", "R3", "P3", "U6", "E4", "Y6", "c4", "A4", "R4", "a6", "C4", "R5",
    "P4", "U7", "A5", "A6", "O5", "L2", "c5", "C5", "Y7", "a7", "A7", "S0", "E6", "R6", "R7", "c6", "P5",
    "C6", "O7", "c7", "C7", "S1", "R8", "R9", "P6", "R10", "R11", "P7", "R12", "R13", "P8", "R14", "R15",
)
KINDS = "YLEOacACPRSUW"


def dot(a, b, ca, cb):
    return lax.dot_general(a, b, (((ca,), (cb,)), ((), ())), preferred_element_type=F32)


def kernel(
    side,
    x_h, dy_h, wg_h, wu_h, wd_h, ug_h, uu_h,
    dx_h, own_d, own_g, own_u, rec_d, rec_g, rec_u, dyl, xl, rl,
    dyt, xt, uo, ux, wdb, wgu, gbuf, zb, dub, accd, accw, pbuf, sin, sout, rsb, rso,
    dyr_s, dyr_r, dyc_s, dyc_r, xr_s, xr_r, xc_s, xc_r, dyt_l, xt_l, u_s, u_r, u_l,
    w_s, w_r, w_l, p_s, p_r, rs_s, rs_r, e_s, e_r, o_l, b_s, b_r, l_s,
):
    _, hb, h = dy_h.shape
    tb = 2 * hb
    q4 = hb // 2
    fb = wg_h.shape[1]
    fh = fb // 2
    m = 2 * side
    me = lax.axis_index("tp")
    chip = me // 2
    core = lax.rem(me, 2)
    other = 1 - core
    py = chip // side
    px = lax.rem(chip, side)
    cls = lax.rem(px + py, side)
    grp = cls // 2
    odd = lax.rem(cls, 2)

    def ring_pos(y, odd_):
        return 2 * lax.rem(side - y, side) + odd_

    def chip_at(g, i):
        k = i // 2
        return lax.rem(side - k, side) * side + lax.rem(k + lax.rem(i, 2) + 2 * g, side)

    def origin(g, pos, d, t):
        return chip_at(g, lax.rem(pos + (2 * m - t if d == 0 else t), m))

    pos = ring_pos(py, odd)
    down = [chip_at(grp, lax.rem(pos + 1, m)) * 2 + core, chip_at(grp, lax.rem(pos + m - 1, m)) * 2 + core]
    sib = chip * 2 + other
    step_ = side - 1 + 2 * odd
    mates = []
    for y, x in ((py, lax.rem(px + step_, side)), (lax.rem(py + step_, side), px)):
        c = lax.rem(x + y, side)
        mates.append(((y * side + x) * 2 + core, c // 2, ring_pos(y, lax.rem(c, 2))))

    leave = [jnp.where(odd == d, mates[1][0], mates[0][0]) for d in range(2)]

    def remote(src, dst, ss, rs, dev):
        return pltpu.make_async_remote_copy(
            src_ref=src, dst_ref=dst, send_sem=ss, recv_sem=rs, device_id={"tp": dev}, device_id_type=MESH
        )

    rows = ((dy_h, dyl, dyr_s, dyr_r, dyc_s, dyc_r, dyt, dyt_l), (x_h, xl, xr_s, xr_r, xc_s, xc_r, xt, xt_l))

    def ring(i, s, d, first=False):
        src, land, ss, rs = rows[i][:4]
        return remote(src.at[d] if first else land.at[s, core, d], land.at[s + 1, core, d], ss.at[s, d], rs.at[s + 1, d], down[d])

    def away(k, d, first=False):
        return remote(x_h.at[d] if first else xl.at[2 * k, core, d], rl.at[k, d], b_s.at[k, d], b_r.at[k, d], leave[d])

    def relay(k, d):
        return remote(rl.at[k, d], xl.at[2 * k + 2, core, d], l_s.at[k, d], xr_r.at[2 * k + 2, d], leave[d])

    def cross(i, s, d, first=False):
        src, land, ss, rs = rows[i][0], rows[i][1], rows[i][4], rows[i][5]
        return remote(src.at[d] if first else land.at[s, core, d], land.at[s, core, d], ss.at[s, d], rs.at[s, d], sib)

    def cross_in(i, s, d):
        land, ss, rs = rows[i][1], rows[i][4], rows[i][5]
        return remote(land.at[s, other, d], land.at[s, other, d], ss.at[s, d], rs.at[s, d], sib)

    def tile_wait(i, t):
        tile, sem = rows[i][6], rows[i][7]
        b = lax.rem(t, 2)
        pltpu.make_async_copy(tile.at[b], tile.at[b], sem.at[b]).wait()

    def tile_load(i, t):
        src, land, tile, sem = rows[i][0], rows[i][1], rows[i][6], rows[i][7]
        b = lax.rem(t, 2)
        for d in range(2):
            cross_in(i, t, d).wait_recv()

        @pl.when(t == 0)
        def _():
            pltpu.make_async_copy(src, tile.at[b, core], sem.at[b]).start()
            pltpu.make_async_copy(land.at[t, other], tile.at[b, other], sem.at[b]).start()

        @pl.when(t > 0)
        def _():
            pltpu.make_async_copy(land.at[t], tile.at[b], sem.at[b]).start()

        if i == 0:
            for d in range(2):
                o = origin(grp, pos, d, t)
                for j, u in enumerate((ug_h, uu_h)):
                    pltpu.make_async_copy(u.at[o, :, d], uo.at[b, j, :, d], u_l.at[b]).start()

    def u_send(t):
        for k, (dev, g, p) in enumerate(mates):
            for d in range(2):
                o = origin(g, p, d, t)
                for j, u in enumerate((ug_h, uu_h)):
                    remote(u.at[o, :, d, :, pl.ds(k * fh, fh)], ux.at[t, k, j, :, d], u_s.at[t, k], u_r.at[t, k], dev).start()

    def u_all(t, k):
        return remote(ux.at[t, k], ux.at[t, k], u_s.at[t, k], u_r.at[t, k], mates[k][0])

    def w_local(i):
        if i == 0:
            return pltpu.make_async_copy(wd_h, wdb.at[pl.ds(0, fb)], w_l.at[i])
        return pltpu.make_async_copy((wg_h, wu_h)[i - 1], wgu.at[:, pl.ds((i - 1) * 2 * fb, fb)], w_l.at[i])

    def w_remote(i, k):
        if i == 0:
            src, dst = wd_h.at[pl.ds(k * fh, fh)], wdb.at[pl.ds(fb + k * fh, fh)]
        else:
            src = (wg_h, wu_h)[i - 1].at[:, pl.ds(k * fh, fh)]
            dst = wgu.at[:, pl.ds((i - 1) * 2 * fb + fb + k * fh, fh)]
        return remote(src, dst, w_s.at[i, k], w_r.at[i, k], mates[k][0])

    def swap(i, k):
        if i == 0:
            src, dst = accd.at[pl.ds(fb + k * fh, fh)], rec_d.at[pl.ds(k * fh, fh)]
        else:
            src = accw.at[:, pl.ds((i - 1) * 2 * fb + fb + k * fh, fh)]
            dst = (rec_g, rec_u)[i - 1].at[:, pl.ds(k * fh, fh)]
        return remote(src, dst, e_s.at[i, k], e_r.at[i, k], mates[k][0])

    def own_out(i):
        if i == 0:
            return pltpu.make_async_copy(accd.at[pl.ds(0, fb)], own_d, o_l.at[0])
        return pltpu.make_async_copy(accw.at[:, pl.ds((i - 1) * 2 * fb, fb)], (own_g, own_u)[i - 1], o_l.at[i])

    def rs_hop(j, d, z):
        a, b = lax.rem(j, 2), lax.rem(j + 1, S)
        return remote(rso.at[a, d, z], rsb.at[b, d, z], rs_s.at[a, d, z], rs_r.at[b, d, z], down[d])

    def part_hop(j):
        a, b = lax.rem(j, 2), lax.rem(j, S)
        return remote(sout.at[a], sin.at[b], p_s.at[a], p_r.at[b], sib)

    barrier = pltpu.get_barrier_semaphore()
    for dev in down + [sib, mates[0][0], mates[1][0]]:
        pl.semaphore_signal(barrier, inc=1, device_id={"tp": dev}, device_id_type=MESH)
    for i in range(3):
        w_local(i).start()
    pl.semaphore_wait(barrier, 5)
    for d in range(2):
        ring(0, 0, d, True).start()
        away(0, d, True).start()
    for d in range(2):
        ring(1, 0, d, True).start()
        cross(0, 0, d, True).start()
        cross(1, 0, d, True).start()

    def zero(i, _):
        accd[pl.ds(pl.multiple_of(i * (2 * fb // 8), 2 * fb // 8), 2 * fb // 8), :] = jnp.zeros((2 * fb // 8, h), F32)
        accw[pl.ds(pl.multiple_of(i * (h // 8), h // 8), h // 8), :] = jnp.zeros((h // 8, 4 * fb), F32)
        return 0

    lax.fori_loop(0, 8, zero, 0)

    ct = min(512, h)
    ht = min(256, h)

    def pass_dy(s):
        for d in range(2):
            ring(0, s - 1, d).wait_recv()

            @pl.when(s < m - 1)
            def _(d=d):
                ring(0, s, d).start()

            cross(0, s, d).start()

    def relay_x(k):
        for d in range(2):
            away(k, d).wait_recv()
            relay(k, d).start()

    def pass_even_x(s):
        k = s // 2
        for d in range(2):
            relay(k - 1, d).wait_recv()

            @pl.when(s < m - 2)
            def _(d=d):
                away(k, d).start()

            ring(1, s, d).start()
            cross(1, s, d).start()

    def take_odd_x(s):
        for d in range(2):
            ring(1, s - 1, d).wait_recv()
            cross(1, s, d).start()

    def grads(t):
        b = lax.rem(t, 2)

        @pl.when(t == 0)
        def _():
            w_local(0).wait()
            for k in range(2):
                w_remote(0, k).wait_recv()

        for k in range(2):
            u_all(t, k).wait_recv()
        pltpu.make_async_copy(uo.at[b], uo.at[b], u_l.at[b]).wait()
        tile_wait(0, t)
        for f in range(2):
            gbuf[:, f * fb:(f + 1) * fb] = dot(dyt[b].reshape(2 * tb, h), wdb[f * fb:(f + 1) * fb, :], 1, 1)

        def act(r, _):
            c, d = r // 2, lax.rem(r, 2)
            rws = pl.ds(pl.multiple_of(r * hb, hb), hb)
            half = pl.ds(pl.multiple_of(d * hb, hb), hb)
            for lo, n, get in (
                (0, fb, lambda j: uo[b, j, c, d]),
                (fb, fh, lambda j: ux[t, 0, j, c, d]),
                (fb + fh, fh, lambda j: ux[t, 1, j, c, d]),
            ):
                g = gbuf[rws, lo:lo + n]
                ug = get(0).astype(F32)
                uu = get(1).astype(F32)
                sg = jax.nn.sigmoid(ug)
                a = ug * sg
                zb[rws, lo:lo + n] = (a * uu).astype(BF16)
                dub[t, c, half, lo:lo + n] = (g * uu * sg * (1.0 + ug * (1.0 - sg))).astype(BF16)
                dub[t, c, half, 2 * fb + lo:2 * fb + lo + n] = (g * a).astype(BF16)
            return 0

        lax.fori_loop(0, 4, act, 0)

        def dwd_tile(j, _):
            cols = pl.ds(pl.multiple_of(j * ct, ct), ct)
            accd[:, cols] += dot(zb[...], dyt[b, :, :, :, cols].reshape(2 * tb, ct), 0, 0)
            return 0

        lax.fori_loop(0, h // ct, dwd_tile, 0)

    def weight_grads(t):
        b = lax.rem(t, 2)

        tile_wait(1, t)

        def dw_tile(j, _):
            cols = pl.ds(pl.multiple_of(j * ht, ht), ht)
            accw[cols, :] += dot(xt[b, :, :, :, cols].reshape(2 * tb, ht), dub[t].reshape(2 * tb, 4 * fb), 0, 0)
            return 0

        lax.fori_loop(0, h // ht, dw_tile, 0)

    def partial(j):
        t = lax.rem(j, m)
        b = lax.rem(j, 2)

        @pl.when(j == 1)
        def _():
            for i in (1, 2):
                w_local(i).wait()
                for k in range(2):
                    w_remote(i, k).wait_recv()

        @pl.when(j >= 3)
        def _():
            part_hop(j - 2).wait_send()

        def send_tile(c, _):
            cols = pl.ds(pl.multiple_of(c * ct, ct), ct)
            sout[b, :, cols] = dot(dub[t, other], wgu[cols, :], 1, 1).astype(BF16)
            return 0

        lax.fori_loop(0, h // ct, send_tile, 0)

        def keep_tile(c, _):
            cols = pl.ds(pl.multiple_of(c * ct, ct), ct)
            pbuf[b, :, cols] = dot(dub[t, core], wgu[cols, :], 1, 1)
            return 0

        lax.fori_loop(0, h // ct, keep_tile, 0)
        part_hop(j).start()

    def total(j, d, z, first):
        lo = pl.multiple_of(d * hb + z * q4, q4)
        v = pbuf[lax.rem(j, 2), pl.ds(lo, q4), :] + sin[lax.rem(j, S), pl.ds(lo, q4), :].astype(F32)
        if not first:
            v = v + rsb[lax.rem(j, S), d, z].astype(F32)
        return v.astype(BF16)

    def pass_sum(i):
        j, z = i // 2, lax.rem(i, 2)

        @pl.when(z == 0)
        def _():
            part_hop(j).wait_recv()

        @pl.when(j >= 3)
        def _():
            for d in range(2):
                rs_hop(j - 2, d, z).wait_send()

        @pl.when(j >= 2)
        def _():
            for d in range(2):
                rs_hop(j - 1, d, z).wait_recv()
                rso[lax.rem(j, 2), d, z] = total(j, d, z, False)

        @pl.when(j == 1)
        def _():
            for d in range(2):
                rso[lax.rem(j, 2), d, z] = total(j, d, z, True)

        for d in range(2):
            rs_hop(j, d, z).start()

    def swaps(i):
        for which in ((0,), (1, 2)):
            @pl.when(i == which[0])
            def _(which=which):
                for w in which:
                    for k in range(2):
                        swap(w, k).start()
                    own_out(w).start()

    def send_weight(i):
        for w in range(3):
            @pl.when(i == w)
            def _(w=w):
                for k in range(2):
                    w_remote(w, k).start()

    work = dict(
        Y=pass_dy, L=relay_x, E=pass_even_x, O=take_odd_x, a=lambda t: tile_load(0, t), c=lambda t: tile_load(1, t),
        A=grads, C=weight_grads, P=partial, R=pass_sum, S=swaps, U=u_send, W=send_weight,
    )
    packed = [KINDS.index(w[0]) * 16 + int(w[1:]) for w in PLAN]

    def step(i, _):
        op = jnp.int32(packed[0])
        for k, code in enumerate(packed[1:], 1):
            op = jnp.where(i == k, code, op)
        kind, arg = op // 16, lax.rem(op, 16)
        for k, name in enumerate(KINDS):
            @pl.when(kind == k)
            def _(name=name):
                work[name](arg)
        return 0

    lax.fori_loop(0, len(packed), step, 0)

    part_hop(m).wait_recv()
    outs = []
    for d in range(2):
        for z in range(2):
            rs_hop(m - 2, d, z).wait_send()
    for z in range(2):
        for d in range(2):
            rs_hop(m - 1, d, z).wait_recv()
            rso[m % 2, d, z] = total(m, d, z, False)
            outs.append(pltpu.make_async_copy(rso.at[m % 2, d, z], dx_h.at[pl.ds(d * hb + z * q4, q4)], o_l.at[3 + 2 * d + z]))
            outs[-1].start()

    for i in range(3):
        own_out(i).wait()
        for k in range(2):
            swap(i, k).wait()
            w_remote(i, k).wait_send()
    for j in (m - 1, m):
        part_hop(j).wait_send()
    for d in range(2):
        for z in range(2):
            rs_hop(m - 1, d, z).wait_send()

    def drain(s, _):
        for k in range(2):
            u_all(s, k).wait_send()
        for i in range(2):
            for d in range(2):
                cross(i, s, d).wait_send()

                @pl.when(s < m - 1 if i == 0 else lax.rem(s, 2) == 0)
                def _(i=i, d=d):
                    ring(i, s, d).wait_send()
        return 0

    lax.fori_loop(0, m, drain, 0)
    for k in range(side - 1):
        for d in range(2):
            away(k, d).wait_send()
            relay(k, d).wait_send()
    for c in outs:
        c.wait()


def solution(mesh):
    tok = P(("dp", "tp"), None)
    col = P(None, "tp")
    row = P("tp", None)
    act = P("dp", "tp")
    n = mesh.shape["tp"] // 2
    side = math.isqrt(n)
    m = 2 * side

    def body(x, dy, wg, wu, wd, ug, uu):
        tb, h = x.shape
        fb = wg.shape[1]
        hb, fh = tb // 2, fb // 2
        vm = pltpu.VMEM
        dma = pltpu.SemaphoreType.DMA
        sds = jax.ShapeDtypeStruct
        flops = 12 * n * tb * h * 2 * fb
        dx, own_d, own_g, own_u, rec_d, rec_g, rec_u, _, _, _ = pl.pallas_call(
            functools.partial(kernel, side),
            out_shape=(
                sds((tb, h), BF16),
                sds((fb, h), F32), sds((h, fb), F32), sds((h, fb), F32),
                sds((fb, h), F32), sds((h, fb), F32), sds((h, fb), F32),
                sds((m, 2, 2, hb, h), BF16), sds((m, 2, 2, hb, h), BF16), sds((side - 1, 2, hb, h), BF16),
            ),
            in_specs=[pl.BlockSpec(memory_space=pltpu.HBM)] * 7,
            out_specs=[pl.BlockSpec(memory_space=pl.ANY)] * 10,
            scratch_shapes=[
                vm((2, 2, 2, hb, h), BF16),
                vm((2, 2, 2, hb, h), BF16),
                vm((2, 2, 2, 2, hb, fb), BF16),
                vm((m, 2, 2, 2, 2, hb, fh), BF16),
                vm((2 * fb, h), BF16),
                vm((h, 4 * fb), BF16),
                vm((2 * tb, 2 * fb), F32),
                vm((2 * tb, 2 * fb), BF16),
                vm((m, 2, tb, 4 * fb), BF16),
                vm((2 * fb, h), F32),
                vm((h, 4 * fb), F32),
                vm((2, tb, h), F32),
                vm((S, tb, h), BF16),
                vm((2, tb, h), BF16),
                vm((S, 2, 2, hb // 2, h), BF16),
                vm((2, 2, 2, hb // 2, h), BF16),
                dma((m, 2)), dma((m, 2)), dma((m, 2)), dma((m, 2)),
                dma((m, 2)), dma((m, 2)), dma((m, 2)), dma((m, 2)),
                dma((2,)), dma((2,)), dma((m, 2)), dma((m, 2)), dma((2,)),
                dma((3, 2)), dma((3, 2)), dma((3,)), dma((2,)), dma((S,)),
                dma((2, 2, 2)), dma((S, 2, 2)), dma((3, 2)), dma((3, 2)), dma((7,)),
                dma((side - 1, 2)), dma((side - 1, 2)), dma((side - 1, 2)),
            ],
            compiler_params=pltpu.CompilerParams(
                collective_id=0, has_side_effects=True, vmem_limit_bytes=62 * 1024 * 1024
            ),
            cost_estimate=pl.CostEstimate(flops=flops, bytes_accessed=2 * flops // 1000, transcendentals=0),
        )(
            x.reshape(2, hb, h), dy.reshape(2, hb, h), wg, wu, wd,
            ug.reshape(n, 2, 2, hb, fb), uu.reshape(n, 2, 2, hb, fb),
        )
        return dx, own_g + rec_g, own_u + rec_u, own_d + rec_d

    return jax.shard_map(
        body, mesh=mesh, in_specs=(tok, tok, col, col, row, act, act), out_specs=(tok, act, act, tok), check_vma=False
    )
```

```python
import functools
import math

import jax
import jax.numpy as jnp
from jax import lax
from jax.experimental import pallas as pl
from jax.experimental.pallas import tpu as pltpu
from jax.sharding import PartitionSpec as P

F32 = jnp.float32
BF16 = jnp.bfloat16
S = 4
MESH = pl.DeviceIdType.MESH
SPLIT = 3
PLAN = (
    "W1", "U2", "U0", "W0", "Y1", "a0", "a1", "L0", "Y2", "U1", "Y3", "W2", "A0", "c0", "E2", "a2", "C0",
    "U3", "O1", "A1", "c1", "Y4", "A2", "P1", "R2", "P2", "a3", "L1", "U4", "Y5", "R3", "U5", "c2", "C1",
    "A3", "a4", "C2", "E4", "O3", "c3", "Y6", "c4", "U6", "P3", "C3", "a5", "A4", "O5", "U7", "R4", "A5",
    "C4", "a6", "L2", "R5", "Y7", "A6", "a7", "A7", "c5", "E6", "S0", "C5", "c6", "P4", "R6", "C6", "O7",
    "c7", "R7", "C7", "R8", "S1", "P5", "R9", "R10", "P6", "R11", "R12", "P7", "R13", "R14", "P8", "R15",
)
KINDS = "YLEOacACPRSUW"


def dot(a, b, ca, cb):
    return lax.dot_general(a, b, (((ca,), (cb,)), ((), ())), preferred_element_type=F32)


def kernel(
    side,
    x_h, dy_h, wg_h, wu_h, wd_h, ug_h, uu_h,
    dx_h, own_d, own_g, own_u, rec_d, rec_g, rec_u, dyl, xl, rl,
    dyt, xt, uo, ux, wdb, wgu, gbuf, zb, dub, accd, accw, pbuf, sin, sout, rsb, rso,
    dyr_s, dyr_r, dyc_s, dyc_r, xr_s, xr_r, xc_s, xc_r, dyt_l, xt_l, u_s, u_r, u_l,
    w_s, w_r, w_l, p_s, p_r, rs_s, rs_r, e_s, e_r, o_l, b_s, b_r, l_s,
):
    _, hb, h = dy_h.shape
    tb = 2 * hb
    q4 = hb // 2
    fb = wg_h.shape[1]
    fh = fb // 2
    m = 2 * side
    me = lax.axis_index("tp")
    chip = me // 2
    core = lax.rem(me, 2)
    other = 1 - core
    py = chip // side
    px = lax.rem(chip, side)
    cls = lax.rem(px + py, side)
    grp = cls // 2
    odd = lax.rem(cls, 2)

    def ring_pos(y, odd_):
        return 2 * lax.rem(side - y, side) + odd_

    def chip_at(g, i):
        k = i // 2
        return lax.rem(side - k, side) * side + lax.rem(k + lax.rem(i, 2) + 2 * g, side)

    def origin(g, pos, d, t):
        return chip_at(g, lax.rem(pos + (2 * m - t if d == 0 else t), m))

    pos = ring_pos(py, odd)
    down = [chip_at(grp, lax.rem(pos + 1, m)) * 2 + core, chip_at(grp, lax.rem(pos + m - 1, m)) * 2 + core]
    sib = chip * 2 + other
    step_ = side - 1 + 2 * odd
    mates = []
    for y, x in ((py, lax.rem(px + step_, side)), (lax.rem(py + step_, side), px)):
        c = lax.rem(x + y, side)
        mates.append(((y * side + x) * 2 + core, c // 2, ring_pos(y, lax.rem(c, 2))))

    leave = [jnp.where(odd == d, mates[1][0], mates[0][0]) for d in range(2)]

    def remote(src, dst, ss, rs, dev):
        return pltpu.make_async_remote_copy(
            src_ref=src, dst_ref=dst, send_sem=ss, recv_sem=rs, device_id={"tp": dev}, device_id_type=MESH
        )

    rows = ((dy_h, dyl, dyr_s, dyr_r, dyc_s, dyc_r, dyt, dyt_l), (x_h, xl, xr_s, xr_r, xc_s, xc_r, xt, xt_l))

    def ring(i, s, d, first=False):
        src, land, ss, rs = rows[i][:4]
        return remote(src.at[d] if first else land.at[s, core, d], land.at[s + 1, core, d], ss.at[s, d], rs.at[s + 1, d], down[d])

    last = side - 2
    hz = SPLIT * hb // 4

    def spill(d):
        s, rws = m - 3, pl.ds(hz, hb - hz)
        return remote(xl.at[s, core, d, rws], xl.at[s + 1, core, d, rws], xr_s.at[s, d], xr_r.at[0, d], down[d])

    def away(k, d, first=False, part=False):
        rws = pl.ds(0, hz if part else hb)
        src = x_h.at[d] if first else xl.at[2 * k, core, d, rws]
        return remote(src, rl.at[k, d, rws], b_s.at[k, d], b_r.at[k, d], leave[d])

    def relay(k, d, part=False):
        rws = pl.ds(0, hz if part else hb)
        return remote(rl.at[k, d, rws], xl.at[2 * k + 2, core, d, rws], l_s.at[k, d], xr_r.at[2 * k + 2, d], leave[d])

    def cross(i, s, d, first=False):
        src, land, ss, rs = rows[i][0], rows[i][1], rows[i][4], rows[i][5]
        return remote(src.at[d] if first else land.at[s, core, d], land.at[s, core, d], ss.at[s, d], rs.at[s, d], sib)

    def cross_in(i, s, d):
        land, ss, rs = rows[i][1], rows[i][4], rows[i][5]
        return remote(land.at[s, other, d], land.at[s, other, d], ss.at[s, d], rs.at[s, d], sib)

    def tile_wait(i, t):
        tile, sem = rows[i][6], rows[i][7]
        b = lax.rem(t, 2)
        pltpu.make_async_copy(tile.at[b], tile.at[b], sem.at[b]).wait()

    def tile_load(i, t):
        src, land, tile, sem = rows[i][0], rows[i][1], rows[i][6], rows[i][7]
        b = lax.rem(t, 2)
        for d in range(2):
            cross_in(i, t, d).wait_recv()

        @pl.when(t == 0)
        def _():
            pltpu.make_async_copy(src, tile.at[b, core], sem.at[b]).start()
            pltpu.make_async_copy(land.at[t, other], tile.at[b, other], sem.at[b]).start()

        @pl.when(t > 0)
        def _():
            pltpu.make_async_copy(land.at[t], tile.at[b], sem.at[b]).start()

        if i == 0:
            for d in range(2):
                o = origin(grp, pos, d, t)
                for j, u in enumerate((ug_h, uu_h)):
                    pltpu.make_async_copy(u.at[o, :, d], uo.at[b, j, :, d], u_l.at[b]).start()

    def u_send(t):
        for k, (dev, g, p) in enumerate(mates):
            for d in range(2):
                o = origin(g, p, d, t)
                for j, u in enumerate((ug_h, uu_h)):
                    remote(u.at[o, :, d, :, pl.ds(k * fh, fh)], ux.at[t, k, j, :, d], u_s.at[t, k], u_r.at[t, k], dev).start()

    def u_all(t, k):
        return remote(ux.at[t, k], ux.at[t, k], u_s.at[t, k], u_r.at[t, k], mates[k][0])

    def w_local(i):
        if i == 0:
            return pltpu.make_async_copy(wd_h, wdb.at[pl.ds(0, fb)], w_l.at[i])
        return pltpu.make_async_copy((wg_h, wu_h)[i - 1], wgu.at[:, pl.ds((i - 1) * 2 * fb, fb)], w_l.at[i])

    def w_remote(i, k):
        if i == 0:
            src, dst = wd_h.at[pl.ds(k * fh, fh)], wdb.at[pl.ds(fb + k * fh, fh)]
        else:
            src = (wg_h, wu_h)[i - 1].at[:, pl.ds(k * fh, fh)]
            dst = wgu.at[:, pl.ds((i - 1) * 2 * fb + fb + k * fh, fh)]
        return remote(src, dst, w_s.at[i, k], w_r.at[i, k], mates[k][0])

    def swap(i, k):
        if i == 0:
            src, dst = accd.at[pl.ds(fb + k * fh, fh)], rec_d.at[pl.ds(k * fh, fh)]
        else:
            src = accw.at[:, pl.ds((i - 1) * 2 * fb + fb + k * fh, fh)]
            dst = (rec_g, rec_u)[i - 1].at[:, pl.ds(k * fh, fh)]
        return remote(src, dst, e_s.at[i, k], e_r.at[i, k], mates[k][0])

    def own_out(i):
        if i == 0:
            return pltpu.make_async_copy(accd.at[pl.ds(0, fb)], own_d, o_l.at[0])
        return pltpu.make_async_copy(accw.at[:, pl.ds((i - 1) * 2 * fb, fb)], (own_g, own_u)[i - 1], o_l.at[i])

    def rs_hop(j, d, z):
        a, b = lax.rem(j, 2), lax.rem(j + 1, S)
        return remote(rso.at[a, d, z], rsb.at[b, d, z], rs_s.at[a, d, z], rs_r.at[b, d, z], down[d])

    def part_hop(j):
        a, b = lax.rem(j, 2), lax.rem(j, S)
        return remote(sout.at[a], sin.at[b], p_s.at[a], p_r.at[b], sib)

    barrier = pltpu.get_barrier_semaphore()
    for dev in down + [sib, mates[0][0], mates[1][0]]:
        pl.semaphore_signal(barrier, inc=1, device_id={"tp": dev}, device_id_type=MESH)
    for i in range(3):
        w_local(i).start()
    pl.semaphore_wait(barrier, 5)
    for d in range(2):
        ring(0, 0, d, True).start()
        away(0, d, True).start()
    for d in range(2):
        ring(1, 0, d, True).start()
        cross(0, 0, d, True).start()
        cross(1, 0, d, True).start()

    def zero(i, _):
        accd[pl.ds(pl.multiple_of(i * (2 * fb // 8), 2 * fb // 8), 2 * fb // 8), :] = jnp.zeros((2 * fb // 8, h), F32)
        accw[pl.ds(pl.multiple_of(i * (h // 8), h // 8), h // 8), :] = jnp.zeros((h // 8, 4 * fb), F32)
        return 0

    lax.fori_loop(0, 8, zero, 0)

    ct = min(512, h)
    ht = min(256, h)

    def pass_dy(s):
        for d in range(2):
            ring(0, s - 1, d).wait_recv()

            @pl.when(s < m - 1)
            def _(d=d):
                ring(0, s, d).start()

            cross(0, s, d).start()

    def relay_x(k):
        for part in (False, True):
            @pl.when((k == last) == part)
            def _(part=part):
                for d in range(2):
                    away(k, d, part=part).wait_recv()
                    relay(k, d, part).start()

    def pass_even_x(s):
        k = s // 2
        for d in range(2):
            @pl.when(k - 1 < last)
            def _(d=d):
                relay(k - 1, d).wait_recv()

            @pl.when(k - 1 == last)
            def _(d=d):
                relay(k - 1, d, True).wait_recv()
                spill(d).wait_recv()

            @pl.when(k < last)
            def _(d=d):
                away(k, d).start()

            @pl.when(k == last)
            def _(d=d):
                away(k, d, part=True).start()

            ring(1, s, d).start()
            cross(1, s, d).start()

    def take_odd_x(s):
        for d in range(2):
            ring(1, s - 1, d).wait_recv()

            @pl.when(s == m - 3)
            def _(d=d):
                spill(d).start()

            cross(1, s, d).start()

    def grads(t):
        b = lax.rem(t, 2)

        @pl.when(t == 0)
        def _():
            w_local(0).wait()
            for k in range(2):
                w_remote(0, k).wait_recv()

        for k in range(2):
            u_all(t, k).wait_recv()
        pltpu.make_async_copy(uo.at[b], uo.at[b], u_l.at[b]).wait()
        tile_wait(0, t)
        for f in range(2):
            gbuf[:, f * fb:(f + 1) * fb] = dot(dyt[b].reshape(2 * tb, h), wdb[f * fb:(f + 1) * fb, :], 1, 1)

        def act(r, _):
            c, d = r // 2, lax.rem(r, 2)
            rws = pl.ds(pl.multiple_of(r * hb, hb), hb)
            half = pl.ds(pl.multiple_of(d * hb, hb), hb)
            for lo, n, get in (
                (0, fb, lambda j: uo[b, j, c, d]),
                (fb, fh, lambda j: ux[t, 0, j, c, d]),
                (fb + fh, fh, lambda j: ux[t, 1, j, c, d]),
            ):
                g = gbuf[rws, lo:lo + n]
                ug = get(0).astype(F32)
                uu = get(1).astype(F32)
                sg = jax.nn.sigmoid(ug)
                a = ug * sg
                zb[rws, lo:lo + n] = (a * uu).astype(BF16)
                dub[t, c, half, lo:lo + n] = (g * uu * sg * (1.0 + ug * (1.0 - sg))).astype(BF16)
                dub[t, c, half, 2 * fb + lo:2 * fb + lo + n] = (g * a).astype(BF16)
            return 0

        lax.fori_loop(0, 4, act, 0)

        def dwd_tile(j, _):
            cols = pl.ds(pl.multiple_of(j * ct, ct), ct)
            accd[:, cols] += dot(zb[...], dyt[b, :, :, :, cols].reshape(2 * tb, ct), 0, 0)
            return 0

        lax.fori_loop(0, h // ct, dwd_tile, 0)

    def weight_grads(t):
        b = lax.rem(t, 2)

        tile_wait(1, t)

        def dw_tile(j, _):
            cols = pl.ds(pl.multiple_of(j * ht, ht), ht)
            accw[cols, :] += dot(xt[b, :, :, :, cols].reshape(2 * tb, ht), dub[t].reshape(2 * tb, 4 * fb), 0, 0)
            return 0

        lax.fori_loop(0, h // ht, dw_tile, 0)

    def partial(j):
        t = lax.rem(j, m)
        b = lax.rem(j, 2)

        @pl.when(j == 1)
        def _():
            for i in (1, 2):
                w_local(i).wait()
                for k in range(2):
                    w_remote(i, k).wait_recv()

        @pl.when(j >= 3)
        def _():
            part_hop(j - 2).wait_send()

        def send_tile(c, _):
            cols = pl.ds(pl.multiple_of(c * ct, ct), ct)
            sout[b, :, cols] = dot(dub[t, other], wgu[cols, :], 1, 1).astype(BF16)
            return 0

        lax.fori_loop(0, h // ct, send_tile, 0)

        def keep_tile(c, _):
            cols = pl.ds(pl.multiple_of(c * ct, ct), ct)
            pbuf[b, :, cols] = dot(dub[t, core], wgu[cols, :], 1, 1)
            return 0

        lax.fori_loop(0, h // ct, keep_tile, 0)
        part_hop(j).start()

    def total(j, d, z, first):
        lo = pl.multiple_of(d * hb + z * q4, q4)
        v = pbuf[lax.rem(j, 2), pl.ds(lo, q4), :] + sin[lax.rem(j, S), pl.ds(lo, q4), :].astype(F32)
        if not first:
            v = v + rsb[lax.rem(j, S), d, z].astype(F32)
        return v.astype(BF16)

    def pass_sum(i):
        j, z = i // 2, lax.rem(i, 2)

        @pl.when(z == 0)
        def _():
            part_hop(j).wait_recv()

        @pl.when(j >= 3)
        def _():
            for d in range(2):
                rs_hop(j - 2, d, z).wait_send()

        @pl.when(j >= 2)
        def _():
            for d in range(2):
                rs_hop(j - 1, d, z).wait_recv()
                rso[lax.rem(j, 2), d, z] = total(j, d, z, False)

        @pl.when(j == 1)
        def _():
            for d in range(2):
                rso[lax.rem(j, 2), d, z] = total(j, d, z, True)

        for d in range(2):
            rs_hop(j, d, z).start()

    def swaps(i):
        for which in ((0,), (1, 2)):
            @pl.when(i == which[0])
            def _(which=which):
                for w in which:
                    for k in range(2):
                        swap(w, k).start()
                    own_out(w).start()

    def send_weight(i):
        for w in range(3):
            @pl.when(i == w)
            def _(w=w):
                for k in range(2):
                    w_remote(w, k).start()

    work = dict(
        Y=pass_dy, L=relay_x, E=pass_even_x, O=take_odd_x, a=lambda t: tile_load(0, t), c=lambda t: tile_load(1, t),
        A=grads, C=weight_grads, P=partial, R=pass_sum, S=swaps, U=u_send, W=send_weight,
    )
    packed = [KINDS.index(w[0]) * 16 + int(w[1:]) for w in PLAN]

    def step(i, _):
        op = jnp.int32(packed[0])
        for k, code in enumerate(packed[1:], 1):
            op = jnp.where(i == k, code, op)
        kind, arg = op // 16, lax.rem(op, 16)
        for k, name in enumerate(KINDS):
            @pl.when(kind == k)
            def _(name=name):
                work[name](arg)
        return 0

    lax.fori_loop(0, len(packed), step, 0)

    part_hop(m).wait_recv()
    outs = []
    for d in range(2):
        for z in range(2):
            rs_hop(m - 2, d, z).wait_send()
    for z in range(2):
        for d in range(2):
            rs_hop(m - 1, d, z).wait_recv()
            rso[m % 2, d, z] = total(m, d, z, False)
            outs.append(pltpu.make_async_copy(rso.at[m % 2, d, z], dx_h.at[pl.ds(d * hb + z * q4, q4)], o_l.at[3 + 2 * d + z]))
            outs[-1].start()

    for i in range(3):
        own_out(i).wait()
        for k in range(2):
            swap(i, k).wait()
            w_remote(i, k).wait_send()
    for j in (m - 1, m):
        part_hop(j).wait_send()
    for d in range(2):
        for z in range(2):
            rs_hop(m - 1, d, z).wait_send()

    def drain(s, _):
        for k in range(2):
            u_all(s, k).wait_send()
        for i in range(2):
            for d in range(2):
                cross(i, s, d).wait_send()

                @pl.when(s < m - 1 if i == 0 else lax.rem(s, 2) == 0)
                def _(i=i, d=d):
                    ring(i, s, d).wait_send()
        return 0

    lax.fori_loop(0, m, drain, 0)
    for k in range(side - 1):
        for d in range(2):
            away(k, d, part=k == last).wait_send()
            relay(k, d, k == last).wait_send()
    for d in range(2):
        spill(d).wait_send()
    for c in outs:
        c.wait()


def finish(dx, own_d, own_g, own_u, rec_d, rec_g, rec_u, dx_o, d_o, g_o, u_o):
    dx_o[...] = dx[...]
    d_o[...] = own_d[...] + rec_d[...]
    g_o[...] = own_g[...] + rec_g[...]
    u_o[...] = own_u[...] + rec_u[...]


def solution(mesh):
    tok = P(("dp", "tp"), None)
    col = P(None, "tp")
    row = P("tp", None)
    act = P("dp", "tp")
    n = mesh.shape["tp"] // 2
    side = math.isqrt(n)
    m = 2 * side

    def body(x, dy, wg, wu, wd, ug, uu):
        tb, h = x.shape
        fb = wg.shape[1]
        hb, fh = tb // 2, fb // 2
        vm = pltpu.VMEM
        dma = pltpu.SemaphoreType.DMA
        sds = jax.ShapeDtypeStruct
        flops = 12 * n * tb * h * 2 * fb
        dx, own_d, own_g, own_u, rec_d, rec_g, rec_u, _, _, _ = pl.pallas_call(
            functools.partial(kernel, side),
            out_shape=(
                sds((tb, h), BF16),
                sds((fb, h), F32), sds((h, fb), F32), sds((h, fb), F32),
                sds((fb, h), F32), sds((h, fb), F32), sds((h, fb), F32),
                sds((m, 2, 2, hb, h), BF16), sds((m, 2, 2, hb, h), BF16), sds((side - 1, 2, hb, h), BF16),
            ),
            in_specs=[pl.BlockSpec(memory_space=pltpu.HBM)] * 7,
            out_specs=[pl.BlockSpec(memory_space=pl.ANY)] * 10,
            scratch_shapes=[
                vm((2, 2, 2, hb, h), BF16),
                vm((2, 2, 2, hb, h), BF16),
                vm((2, 2, 2, 2, hb, fb), BF16),
                vm((m, 2, 2, 2, 2, hb, fh), BF16),
                vm((2 * fb, h), BF16),
                vm((h, 4 * fb), BF16),
                vm((2 * tb, 2 * fb), F32),
                vm((2 * tb, 2 * fb), BF16),
                vm((m, 2, tb, 4 * fb), BF16),
                vm((2 * fb, h), F32),
                vm((h, 4 * fb), F32),
                vm((2, tb, h), F32),
                vm((S, tb, h), BF16),
                vm((2, tb, h), BF16),
                vm((S, 2, 2, hb // 2, h), BF16),
                vm((2, 2, 2, hb // 2, h), BF16),
                dma((m, 2)), dma((m, 2)), dma((m, 2)), dma((m, 2)),
                dma((m, 2)), dma((m, 2)), dma((m, 2)), dma((m, 2)),
                dma((2,)), dma((2,)), dma((m, 2)), dma((m, 2)), dma((2,)),
                dma((3, 2)), dma((3, 2)), dma((3,)), dma((2,)), dma((S,)),
                dma((2, 2, 2)), dma((S, 2, 2)), dma((3, 2)), dma((3, 2)), dma((7,)),
                dma((side - 1, 2)), dma((side - 1, 2)), dma((side - 1, 2)),
            ],
            compiler_params=pltpu.CompilerParams(
                collective_id=0, has_side_effects=True, vmem_limit_bytes=62 * 1024 * 1024
            ),
            cost_estimate=pl.CostEstimate(flops=flops, bytes_accessed=2 * flops // 1000, transcendentals=0),
        )(
            x.reshape(2, hb, h), dy.reshape(2, hb, h), wg, wu, wd,
            ug.reshape(n, 2, 2, hb, fb), uu.reshape(n, 2, 2, hb, fb),
        )
        grid = 4

        def spec(r, c):
            return pl.BlockSpec((r // grid, c), lambda i: (i, 0))

        dx, dwd, dwg, dwu = pl.pallas_call(
            finish,
            grid=(grid,),
            out_shape=(sds((tb, h), BF16), sds((fb, h), F32), sds((h, fb), F32), sds((h, fb), F32)),
            in_specs=[spec(tb, h)] + [spec(fb, h), spec(h, fb), spec(h, fb)] * 2,
            out_specs=[spec(tb, h), spec(fb, h), spec(h, fb), spec(h, fb)],
        )(dx, own_d, own_g, own_u, rec_d, rec_g, rec_u)
        return dx, dwg, dwu, dwd

    return jax.shard_map(
        body, mesh=mesh, in_specs=(tok, tok, col, col, row, act, act), out_specs=(tok, act, act, tok), check_vma=False
    )
```

```python
import functools
import math

import jax
import jax.numpy as jnp
from jax import lax
from jax.experimental import pallas as pl
from jax.experimental.pallas import tpu as pltpu
from jax.sharding import PartitionSpec as P

F32 = jnp.float32
BF16 = jnp.bfloat16
S = 4
MESH = pl.DeviceIdType.MESH
SPLIT = 6
PLAN = (
    "W1", "U2", "U0", "W0", "Y1", "a0", "a1", "L0", "Y2", "U1", "Y3", "W2", "A0", "c0", "E2", "a2", "C0",
    "U3", "O1", "A1", "c1", "Y4", "A2", "P1", "R2", "P2", "a3", "L1", "U4", "Y5", "R3", "U5", "c2", "C1",
    "A3", "a4", "C2", "E4", "O3", "c3", "Y6", "c4", "U6", "P3", "C3", "a5", "A4", "O5", "U7", "R4", "A5",
    "C4", "a6", "L2", "R5", "Y7", "A6", "a7", "A7", "c5", "E6", "S0", "C5", "c6", "P4", "R6", "C6", "O7",
    "c7", "R7", "C7", "R8", "S1", "P5", "R9", "R10", "P6", "R11", "R12", "P7", "R13", "R14", "P8", "D0", "D1",
    "R15",
)
KINDS = "YLEOacACPRSDUW"


def dot(a, b, ca, cb):
    return lax.dot_general(a, b, (((ca,), (cb,)), ((), ())), preferred_element_type=F32)


def kernel(
    side,
    x_h, dy_h, wg_h, wu_h, wd_h, ug_h, uu_h,
    dx_h, dwd_h, dwg_h, own_u, rec_u, dyl, xl, rl,
    dyt, xt, uo, ux, wdb, wgu, gbuf, zb, dub, accd, accw, pbuf, sin, sout, rsb, rso, rec_d, rec_g,
    dyr_s, dyr_r, dyc_s, dyc_r, xr_s, xr_r, xc_s, xc_r, dyt_l, xt_l, u_s, u_r, u_l,
    w_s, w_r, w_l, p_s, p_r, rs_s, rs_r, e_s, e_r, o_l, b_s, b_r, l_s,
):
    _, hb, h = dy_h.shape
    tb = 2 * hb
    q4 = hb // 2
    fb = wg_h.shape[1]
    fh = fb // 2
    m = 2 * side
    me = lax.axis_index("tp")
    chip = me // 2
    core = lax.rem(me, 2)
    other = 1 - core
    py = chip // side
    px = lax.rem(chip, side)
    cls = lax.rem(px + py, side)
    grp = cls // 2
    odd = lax.rem(cls, 2)

    def ring_pos(y, odd_):
        return 2 * lax.rem(side - y, side) + odd_

    def chip_at(g, i):
        k = i // 2
        return lax.rem(side - k, side) * side + lax.rem(k + lax.rem(i, 2) + 2 * g, side)

    def origin(g, pos, d, t):
        return chip_at(g, lax.rem(pos + (2 * m - t if d == 0 else t), m))

    pos = ring_pos(py, odd)
    down = [chip_at(grp, lax.rem(pos + 1, m)) * 2 + core, chip_at(grp, lax.rem(pos + m - 1, m)) * 2 + core]
    sib = chip * 2 + other
    step_ = side - 1 + 2 * odd
    mates = []
    for y, x in ((py, lax.rem(px + step_, side)), (lax.rem(py + step_, side), px)):
        c = lax.rem(x + y, side)
        mates.append(((y * side + x) * 2 + core, c // 2, ring_pos(y, lax.rem(c, 2))))

    leave = [jnp.where(odd == d, mates[1][0], mates[0][0]) for d in range(2)]

    def remote(src, dst, ss, rs, dev):
        return pltpu.make_async_remote_copy(
            src_ref=src, dst_ref=dst, send_sem=ss, recv_sem=rs, device_id={"tp": dev}, device_id_type=MESH
        )

    rows = ((dy_h, dyl, dyr_s, dyr_r, dyc_s, dyc_r, dyt, dyt_l), (x_h, xl, xr_s, xr_r, xc_s, xc_r, xt, xt_l))

    def ring(i, s, d, first=False):
        src, land, ss, rs = rows[i][:4]
        return remote(src.at[d] if first else land.at[s, core, d], land.at[s + 1, core, d], ss.at[s, d], rs.at[s + 1, d], down[d])

    last = side - 2
    hz = SPLIT * hb // 8

    def spill(d):
        s, rws = m - 3, pl.ds(hz, hb - hz)
        return remote(xl.at[s, core, d, rws], xl.at[s + 1, core, d, rws], xr_s.at[s, d], xr_r.at[0, d], down[d])

    def away(k, d, first=False, part=False):
        rws = pl.ds(0, hz if part else hb)
        src = x_h.at[d] if first else xl.at[2 * k, core, d, rws]
        return remote(src, rl.at[k, d, rws], b_s.at[k, d], b_r.at[k, d], leave[d])

    def relay(k, d, part=False):
        rws = pl.ds(0, hz if part else hb)
        return remote(rl.at[k, d, rws], xl.at[2 * k + 2, core, d, rws], l_s.at[k, d], xr_r.at[2 * k + 2, d], leave[d])

    def cross(i, s, d, first=False):
        src, land, ss, rs = rows[i][0], rows[i][1], rows[i][4], rows[i][5]
        return remote(src.at[d] if first else land.at[s, core, d], land.at[s, core, d], ss.at[s, d], rs.at[s, d], sib)

    def cross_in(i, s, d):
        land, ss, rs = rows[i][1], rows[i][4], rows[i][5]
        return remote(land.at[s, other, d], land.at[s, other, d], ss.at[s, d], rs.at[s, d], sib)

    def tile_wait(i, t):
        tile, sem = rows[i][6], rows[i][7]
        b = lax.rem(t, 2)
        pltpu.make_async_copy(tile.at[b], tile.at[b], sem.at[b]).wait()

    def tile_load(i, t):
        src, land, tile, sem = rows[i][0], rows[i][1], rows[i][6], rows[i][7]
        b = lax.rem(t, 2)
        for d in range(2):
            cross_in(i, t, d).wait_recv()

        @pl.when(t == 0)
        def _():
            pltpu.make_async_copy(src, tile.at[b, core], sem.at[b]).start()
            pltpu.make_async_copy(land.at[t, other], tile.at[b, other], sem.at[b]).start()

        @pl.when(t > 0)
        def _():
            pltpu.make_async_copy(land.at[t], tile.at[b], sem.at[b]).start()

        if i == 0:
            for d in range(2):
                o = origin(grp, pos, d, t)
                for j, u in enumerate((ug_h, uu_h)):
                    pltpu.make_async_copy(u.at[o, :, d], uo.at[b, j, :, d], u_l.at[b]).start()

    def u_send(t):
        for k, (dev, g, p) in enumerate(mates):
            for d in range(2):
                o = origin(g, p, d, t)
                for j, u in enumerate((ug_h, uu_h)):
                    remote(u.at[o, :, d, :, pl.ds(k * fh, fh)], ux.at[t, k, j, :, d], u_s.at[t, k], u_r.at[t, k], dev).start()

    def u_all(t, k):
        return remote(ux.at[t, k], ux.at[t, k], u_s.at[t, k], u_r.at[t, k], mates[k][0])

    def w_local(i):
        if i == 0:
            return pltpu.make_async_copy(wd_h, wdb.at[pl.ds(0, fb)], w_l.at[i])
        return pltpu.make_async_copy((wg_h, wu_h)[i - 1], wgu.at[:, pl.ds((i - 1) * 2 * fb, fb)], w_l.at[i])

    def w_remote(i, k):
        if i == 0:
            src, dst = wd_h.at[pl.ds(k * fh, fh)], wdb.at[pl.ds(fb + k * fh, fh)]
        else:
            src = (wg_h, wu_h)[i - 1].at[:, pl.ds(k * fh, fh)]
            dst = wgu.at[:, pl.ds((i - 1) * 2 * fb + fb + k * fh, fh)]
        return remote(src, dst, w_s.at[i, k], w_r.at[i, k], mates[k][0])

    def swap(i, k):
        if i == 0:
            src, dst = accd.at[pl.ds(fb + k * fh, fh)], rec_d.at[pl.ds(k * fh, fh)]
        else:
            src = accw.at[:, pl.ds((i - 1) * 2 * fb + fb + k * fh, fh)]
            dst = (rec_g, rec_u)[i - 1].at[:, pl.ds(k * fh, fh)]
        return remote(src, dst, e_s.at[i, k], e_r.at[i, k], mates[k][0])

    def own_out(i):
        if i == 0:
            return pltpu.make_async_copy(accd.at[pl.ds(0, fb)], dwd_h, o_l.at[0])
        return pltpu.make_async_copy(accw.at[:, pl.ds((i - 1) * 2 * fb, fb)], (dwg_h, own_u)[i - 1], o_l.at[i])

    def rs_hop(j, d, z):
        a, b = lax.rem(j, 2), lax.rem(j + 1, S)
        return remote(rso.at[a, d, z], rsb.at[b, d, z], rs_s.at[a, d, z], rs_r.at[b, d, z], down[d])

    def part_hop(j):
        a, b = lax.rem(j, 2), lax.rem(j, S)
        return remote(sout.at[a], sin.at[b], p_s.at[a], p_r.at[b], sib)

    barrier = pltpu.get_barrier_semaphore()
    for dev in down + [sib, mates[0][0], mates[1][0]]:
        pl.semaphore_signal(barrier, inc=1, device_id={"tp": dev}, device_id_type=MESH)
    for i in range(3):
        w_local(i).start()
    pl.semaphore_wait(barrier, 5)
    for d in range(2):
        ring(0, 0, d, True).start()
        away(0, d, True).start()
    for d in range(2):
        ring(1, 0, d, True).start()
        cross(0, 0, d, True).start()
        cross(1, 0, d, True).start()

    def zero(i, _):
        accd[pl.ds(pl.multiple_of(i * (2 * fb // 8), 2 * fb // 8), 2 * fb // 8), :] = jnp.zeros((2 * fb // 8, h), F32)
        accw[pl.ds(pl.multiple_of(i * (h // 8), h // 8), h // 8), :] = jnp.zeros((h // 8, 4 * fb), F32)
        return 0

    lax.fori_loop(0, 8, zero, 0)

    ct = min(512, h)
    ht = min(256, h)

    def pass_dy(s):
        for d in range(2):
            ring(0, s - 1, d).wait_recv()

            @pl.when(s < m - 1)
            def _(d=d):
                ring(0, s, d).start()

            cross(0, s, d).start()

    def relay_x(k):
        for part in (False, True):
            @pl.when((k == last) == part)
            def _(part=part):
                for d in range(2):
                    away(k, d, part=part).wait_recv()
                    relay(k, d, part).start()

    def pass_even_x(s):
        k = s // 2
        for d in range(2):
            @pl.when(k - 1 < last)
            def _(d=d):
                relay(k - 1, d).wait_recv()

            @pl.when(k - 1 == last)
            def _(d=d):
                relay(k - 1, d, True).wait_recv()
                spill(d).wait_recv()

            @pl.when(k < last)
            def _(d=d):
                away(k, d).start()

            @pl.when(k == last)
            def _(d=d):
                away(k, d, part=True).start()

            ring(1, s, d).start()
            cross(1, s, d).start()

    def take_odd_x(s):
        for d in range(2):
            ring(1, s - 1, d).wait_recv()

            @pl.when(s == m - 3)
            def _(d=d):
                spill(d).start()

            cross(1, s, d).start()

    def grads(t):
        b = lax.rem(t, 2)

        @pl.when(t == 0)
        def _():
            w_local(0).wait()
            for k in range(2):
                w_remote(0, k).wait_recv()

        for k in range(2):
            u_all(t, k).wait_recv()
        pltpu.make_async_copy(uo.at[b], uo.at[b], u_l.at[b]).wait()
        tile_wait(0, t)
        for f in range(2):
            gbuf[:, f * fb:(f + 1) * fb] = dot(dyt[b].reshape(2 * tb, h), wdb[f * fb:(f + 1) * fb, :], 1, 1)

        def act(r, _):
            c, d = r // 2, lax.rem(r, 2)
            rws = pl.ds(pl.multiple_of(r * hb, hb), hb)
            half = pl.ds(pl.multiple_of(d * hb, hb), hb)
            for lo, n, get in (
                (0, fb, lambda j: uo[b, j, c, d]),
                (fb, fh, lambda j: ux[t, 0, j, c, d]),
                (fb + fh, fh, lambda j: ux[t, 1, j, c, d]),
            ):
                g = gbuf[rws, lo:lo + n]
                ug = get(0).astype(F32)
                uu = get(1).astype(F32)
                sg = jax.nn.sigmoid(ug)
                a = ug * sg
                zb[rws, lo:lo + n] = (a * uu).astype(BF16)
                dub[t, c, half, lo:lo + n] = (g * uu * sg * (1.0 + ug * (1.0 - sg))).astype(BF16)
                dub[t, c, half, 2 * fb + lo:2 * fb + lo + n] = (g * a).astype(BF16)
            return 0

        lax.fori_loop(0, 4, act, 0)

        def dwd_tile(j, _):
            cols = pl.ds(pl.multiple_of(j * ct, ct), ct)
            accd[:, cols] += dot(zb[...], dyt[b, :, :, :, cols].reshape(2 * tb, ct), 0, 0)
            return 0

        lax.fori_loop(0, h // ct, dwd_tile, 0)

    def weight_grads(t):
        b = lax.rem(t, 2)

        tile_wait(1, t)

        def dw_tile(j, _):
            cols = pl.ds(pl.multiple_of(j * ht, ht), ht)
            accw[cols, :] += dot(xt[b, :, :, :, cols].reshape(2 * tb, ht), dub[t].reshape(2 * tb, 4 * fb), 0, 0)
            return 0

        lax.fori_loop(0, h // ht, dw_tile, 0)

    def partial(j):
        t = lax.rem(j, m)
        b = lax.rem(j, 2)

        @pl.when(j == 1)
        def _():
            for i in (1, 2):
                w_local(i).wait()
                for k in range(2):
                    w_remote(i, k).wait_recv()

        @pl.when(j >= 3)
        def _():
            part_hop(j - 2).wait_send()

        def send_tile(c, _):
            cols = pl.ds(pl.multiple_of(c * ct, ct), ct)
            sout[b, :, cols] = dot(dub[t, other], wgu[cols, :], 1, 1).astype(BF16)
            return 0

        lax.fori_loop(0, h // ct, send_tile, 0)

        def keep_tile(c, _):
            cols = pl.ds(pl.multiple_of(c * ct, ct), ct)
            pbuf[b, :, cols] = dot(dub[t, core], wgu[cols, :], 1, 1)
            return 0

        lax.fori_loop(0, h // ct, keep_tile, 0)
        part_hop(j).start()

    def total(j, d, z, first):
        lo = pl.multiple_of(d * hb + z * q4, q4)
        v = pbuf[lax.rem(j, 2), pl.ds(lo, q4), :] + sin[lax.rem(j, S), pl.ds(lo, q4), :].astype(F32)
        if not first:
            v = v + rsb[lax.rem(j, S), d, z].astype(F32)
        return v.astype(BF16)

    def pass_sum(i):
        j, z = i // 2, lax.rem(i, 2)

        @pl.when(z == 0)
        def _():
            part_hop(j).wait_recv()

        @pl.when(j >= 3)
        def _():
            for d in range(2):
                rs_hop(j - 2, d, z).wait_send()

        @pl.when(j >= 2)
        def _():
            for d in range(2):
                rs_hop(j - 1, d, z).wait_recv()
                rso[lax.rem(j, 2), d, z] = total(j, d, z, False)

        @pl.when(j == 1)
        def _():
            for d in range(2):
                rso[lax.rem(j, 2), d, z] = total(j, d, z, True)

        for d in range(2):
            rs_hop(j, d, z).start()

    def swaps(i):
        for which in ((0,), (1, 2)):
            @pl.when(i == which[0])
            def _(which=which):
                for w in which:
                    for k in range(2):
                        swap(w, k).start()
                    if w == 2:
                        own_out(w).start()

    def fold(i):
        @pl.when(i == 0)
        def _():
            for k in range(2):
                swap(0, k).wait_recv()
            accd[0:fb, :] += rec_d[...]
            own_out(0).start()

        @pl.when(i == 1)
        def _():
            for k in range(2):
                swap(1, k).wait_recv()
            accw[:, 0:fb] += rec_g[...]
            own_out(1).start()

    def send_weight(i):
        for w in range(3):
            @pl.when(i == w)
            def _(w=w):
                for k in range(2):
                    w_remote(w, k).start()

    work = dict(
        Y=pass_dy, L=relay_x, E=pass_even_x, O=take_odd_x, a=lambda t: tile_load(0, t), c=lambda t: tile_load(1, t),
        A=grads, C=weight_grads, P=partial, R=pass_sum, S=swaps, D=fold, U=u_send, W=send_weight,
    )
    packed = [KINDS.index(w[0]) * 16 + int(w[1:]) for w in PLAN]

    def step(i, _):
        op = jnp.int32(packed[0])
        for k, code in enumerate(packed[1:], 1):
            op = jnp.where(i == k, code, op)
        kind, arg = op // 16, lax.rem(op, 16)
        for k, name in enumerate(KINDS):
            @pl.when(kind == k)
            def _(name=name):
                work[name](arg)
        return 0

    lax.fori_loop(0, len(packed), step, 0)

    part_hop(m).wait_recv()
    outs = []
    for d in range(2):
        for z in range(2):
            rs_hop(m - 2, d, z).wait_send()
    for z in range(2):
        for d in range(2):
            rs_hop(m - 1, d, z).wait_recv()
            rso[m % 2, d, z] = total(m, d, z, False)
            outs.append(pltpu.make_async_copy(rso.at[m % 2, d, z], dx_h.at[pl.ds(d * hb + z * q4, q4)], o_l.at[3 + 2 * d + z]))
            outs[-1].start()

    for i in range(3):
        own_out(i).wait()
        for k in range(2):
            swap(i, k).wait_send()
            if i == 2:
                swap(i, k).wait_recv()
            w_remote(i, k).wait_send()
    for j in (m - 1, m):
        part_hop(j).wait_send()
    for d in range(2):
        for z in range(2):
            rs_hop(m - 1, d, z).wait_send()

    def drain(s, _):
        for k in range(2):
            u_all(s, k).wait_send()
        for i in range(2):
            for d in range(2):
                cross(i, s, d).wait_send()

                @pl.when(s < m - 1 if i == 0 else lax.rem(s, 2) == 0)
                def _(i=i, d=d):
                    ring(i, s, d).wait_send()
        return 0

    lax.fori_loop(0, m, drain, 0)
    for k in range(side - 1):
        for d in range(2):
            away(k, d, part=k == last).wait_send()
            relay(k, d, k == last).wait_send()
    for d in range(2):
        spill(d).wait_send()
    for c in outs:
        c.wait()


def finish(dx, dwd, dwg, own_u, rec_u, dx_o, d_o, g_o, u_o):
    dx_o[...] = dx[...]
    d_o[...] = dwd[...]
    g_o[...] = dwg[...]
    u_o[...] = own_u[...] + rec_u[...]


def solution(mesh):
    tok = P(("dp", "tp"), None)
    col = P(None, "tp")
    row = P("tp", None)
    act = P("dp", "tp")
    n = mesh.shape["tp"] // 2
    side = math.isqrt(n)
    m = 2 * side

    def body(x, dy, wg, wu, wd, ug, uu):
        tb, h = x.shape
        fb = wg.shape[1]
        hb, fh = tb // 2, fb // 2
        vm = pltpu.VMEM
        dma = pltpu.SemaphoreType.DMA
        sds = jax.ShapeDtypeStruct
        flops = 12 * n * tb * h * 2 * fb
        dx, dwd, dwg, own_u, rec_u, _, _, _ = pl.pallas_call(
            functools.partial(kernel, side),
            out_shape=(
                sds((tb, h), BF16),
                sds((fb, h), F32), sds((h, fb), F32), sds((h, fb), F32), sds((h, fb), F32),
                sds((m, 2, 2, hb, h), BF16), sds((m, 2, 2, hb, h), BF16), sds((side - 1, 2, hb, h), BF16),
            ),
            in_specs=[pl.BlockSpec(memory_space=pltpu.HBM)] * 7,
            out_specs=[pl.BlockSpec(memory_space=pl.ANY)] * 8,
            scratch_shapes=[
                vm((2, 2, 2, hb, h), BF16),
                vm((2, 2, 2, hb, h), BF16),
                vm((2, 2, 2, 2, hb, fb), BF16),
                vm((m, 2, 2, 2, 2, hb, fh), BF16),
                vm((2 * fb, h), BF16),
                vm((h, 4 * fb), BF16),
                vm((2 * tb, 2 * fb), F32),
                vm((2 * tb, 2 * fb), BF16),
                vm((m, 2, tb, 4 * fb), BF16),
                vm((2 * fb, h), F32),
                vm((h, 4 * fb), F32),
                vm((2, tb, h), F32),
                vm((S, tb, h), BF16),
                vm((2, tb, h), BF16),
                vm((S, 2, 2, hb // 2, h), BF16),
                vm((2, 2, 2, hb // 2, h), BF16),
                vm((fb, h), F32),
                vm((h, fb), F32),
                dma((m, 2)), dma((m, 2)), dma((m, 2)), dma((m, 2)),
                dma((m, 2)), dma((m, 2)), dma((m, 2)), dma((m, 2)),
                dma((2,)), dma((2,)), dma((m, 2)), dma((m, 2)), dma((2,)),
                dma((3, 2)), dma((3, 2)), dma((3,)), dma((2,)), dma((S,)),
                dma((2, 2, 2)), dma((S, 2, 2)), dma((3, 2)), dma((3, 2)), dma((7,)),
                dma((side - 1, 2)), dma((side - 1, 2)), dma((side - 1, 2)),
            ],
            compiler_params=pltpu.CompilerParams(
                collective_id=0, has_side_effects=True, vmem_limit_bytes=62 * 1024 * 1024
            ),
            cost_estimate=pl.CostEstimate(flops=flops, bytes_accessed=2 * flops // 1000, transcendentals=0),
        )(
            x.reshape(2, hb, h), dy.reshape(2, hb, h), wg, wu, wd,
            ug.reshape(n, 2, 2, hb, fb), uu.reshape(n, 2, 2, hb, fb),
        )
        grid = 4

        def spec(r, c):
            return pl.BlockSpec((r // grid, c), lambda i: (i, 0))

        dx, dwd, dwg, dwu = pl.pallas_call(
            finish,
            grid=(grid,),
            out_shape=(sds((tb, h), BF16), sds((fb, h), F32), sds((h, fb), F32), sds((h, fb), F32)),
            in_specs=[spec(tb, h), spec(fb, h)] + [spec(h, fb)] * 3,
            out_specs=[spec(tb, h), spec(fb, h), spec(h, fb), spec(h, fb)],
        )(dx, dwd, dwg, own_u, rec_u)
        return dx, dwg, dwu, dwd

    return jax.shard_map(
        body, mesh=mesh, in_specs=(tok, tok, col, col, row, act, act), out_specs=(tok, act, act, tok), check_vma=False
    )
```

```python
import functools
import math

import jax
import jax.numpy as jnp
from jax import lax
from jax.experimental import pallas as pl
from jax.experimental.pallas import tpu as pltpu
from jax.sharding import PartitionSpec as P

F32 = jnp.float32
BF16 = jnp.bfloat16
S = 4
MESH = pl.DeviceIdType.MESH
SPLIT = (6, 6, 8)
PLAN = (
    "U0", "a0", "W0", "W2", "c0", "Y1", "L0", "A0", "U1", "O1", "a1", "Y2", "c1", "W1", "U2", "C0", "E2",
    "U3", "a2", "Y3", "A1", "O3", "c2", "P1", "Y4", "A2", "L1", "U4", "R2", "U5", "C1", "C2", "R3", "a3",
    "Y5", "a4", "c3", "E4", "A3", "C3", "c4", "A4", "U6", "P2", "Y6", "P3", "a5", "R4", "L2", "A5", "C4",
    "U7", "a6", "A6", "Y7", "E6", "O5", "a7", "R5", "c5", "A7", "S0", "P4", "C5", "c6", "O7", "R6", "c7",
    "C6", "R7", "C7", "R8", "S1", "P5", "D0", "R9", "R10", "P6", "R11", "R12", "P7", "R13", "R14", "D1", "P8",
    "R15",
)
KINDS = "YLEOacACPRSDUW"


def dot(a, b, ca, cb):
    return lax.dot_general(a, b, (((ca,), (cb,)), ((), ())), preferred_element_type=F32)


def kernel(
    side,
    x_h, dy_h, wg_h, wu_h, wd_h, ug_h, uu_h,
    dx_h, dwd_h, dwg_h, own_u, rec_u, dyl, xl, rl,
    dyt, xt, uo, ux, wdb, wgu, gbuf, zb, dub, accd, accw, pbuf, sin, sout, rsb, rso, rec_d, rec_g,
    dyr_s, dyr_r, dyc_s, dyc_r, xr_s, xr_r, xc_s, xc_r, dyt_l, xt_l, u_s, u_r, u_l,
    w_s, w_r, w_l, p_s, p_r, rs_s, rs_r, e_s, e_r, o_l, b_s, b_r, l_s, z_r,
):
    _, hb, h = dy_h.shape
    tb = 2 * hb
    q4 = hb // 2
    fb = wg_h.shape[1]
    fh = fb // 2
    m = 2 * side
    me = lax.axis_index("tp")
    chip = me // 2
    core = lax.rem(me, 2)
    other = 1 - core
    py = chip // side
    px = lax.rem(chip, side)
    cls = lax.rem(px + py, side)
    grp = cls // 2
    odd = lax.rem(cls, 2)

    def ring_pos(y, odd_):
        return 2 * lax.rem(side - y, side) + odd_

    def chip_at(g, i):
        k = i // 2
        return lax.rem(side - k, side) * side + lax.rem(k + lax.rem(i, 2) + 2 * g, side)

    def origin(g, pos, d, t):
        return chip_at(g, lax.rem(pos + (2 * m - t if d == 0 else t), m))

    pos = ring_pos(py, odd)
    down = [chip_at(grp, lax.rem(pos + 1, m)) * 2 + core, chip_at(grp, lax.rem(pos + m - 1, m)) * 2 + core]
    sib = chip * 2 + other
    step_ = side - 1 + 2 * odd
    mates = []
    for y, x in ((py, lax.rem(px + step_, side)), (lax.rem(py + step_, side), px)):
        c = lax.rem(x + y, side)
        mates.append(((y * side + x) * 2 + core, c // 2, ring_pos(y, lax.rem(c, 2))))

    leave = [jnp.where(odd == d, mates[1][0], mates[0][0]) for d in range(2)]

    def remote(src, dst, ss, rs, dev):
        return pltpu.make_async_remote_copy(
            src_ref=src, dst_ref=dst, send_sem=ss, recv_sem=rs, device_id={"tp": dev}, device_id_type=MESH
        )

    rows = ((dy_h, dyl, dyr_s, dyr_r, dyc_s, dyc_r, dyt, dyt_l), (x_h, xl, xr_s, xr_r, xc_s, xc_r, xt, xt_l))

    def ring(i, s, d, first=False):
        src, land, ss, rs = rows[i][:4]
        return remote(src.at[d] if first else land.at[s, core, d], land.at[s + 1, core, d], ss.at[s, d], rs.at[s + 1, d], down[d])

    near = [e * hb // 8 for e in SPLIT]

    def spill(k, d):
        s, rws = 2 * k + 1, pl.ds(near[k], hb - near[k])
        return remote(xl.at[s, core, d, rws], xl.at[s + 1, core, d, rws], xr_s.at[s, d], z_r.at[k, d], down[d])

    def away(k, d, first=False):
        rws = pl.ds(0, near[k])
        src = x_h.at[d, rws] if first else xl.at[2 * k, core, d, rws]
        return remote(src, rl.at[k, d, rws], b_s.at[k, d], b_r.at[k, d], leave[d])

    def relay(k, d):
        rws = pl.ds(0, near[k])
        return remote(rl.at[k, d, rws], xl.at[2 * k + 2, core, d, rws], l_s.at[k, d], xr_r.at[2 * k + 2, d], leave[d])

    def cross(i, s, d, first=False):
        src, land, ss, rs = rows[i][0], rows[i][1], rows[i][4], rows[i][5]
        return remote(src.at[d] if first else land.at[s, core, d], land.at[s, core, d], ss.at[s, d], rs.at[s, d], sib)

    def cross_in(i, s, d):
        land, ss, rs = rows[i][1], rows[i][4], rows[i][5]
        return remote(land.at[s, other, d], land.at[s, other, d], ss.at[s, d], rs.at[s, d], sib)

    def tile_wait(i, t):
        tile, sem = rows[i][6], rows[i][7]
        b = lax.rem(t, 2)
        pltpu.make_async_copy(tile.at[b], tile.at[b], sem.at[b]).wait()

    def tile_load(i, t):
        src, land, tile, sem = rows[i][0], rows[i][1], rows[i][6], rows[i][7]
        b = lax.rem(t, 2)
        for d in range(2):
            cross_in(i, t, d).wait_recv()

        @pl.when(t == 0)
        def _():
            pltpu.make_async_copy(src, tile.at[b, core], sem.at[b]).start()
            pltpu.make_async_copy(land.at[t, other], tile.at[b, other], sem.at[b]).start()

        @pl.when(t > 0)
        def _():
            pltpu.make_async_copy(land.at[t], tile.at[b], sem.at[b]).start()

        if i == 0:
            for d in range(2):
                o = origin(grp, pos, d, t)
                for j, u in enumerate((ug_h, uu_h)):
                    pltpu.make_async_copy(u.at[o, :, d], uo.at[b, j, :, d], u_l.at[b]).start()

    def u_send(t):
        for k, (dev, g, p) in enumerate(mates):
            for d in range(2):
                o = origin(g, p, d, t)
                for j, u in enumerate((ug_h, uu_h)):
                    remote(u.at[o, :, d, :, pl.ds(k * fh, fh)], ux.at[t, k, j, :, d], u_s.at[t, k], u_r.at[t, k], dev).start()

    def u_all(t, k):
        return remote(ux.at[t, k], ux.at[t, k], u_s.at[t, k], u_r.at[t, k], mates[k][0])

    def w_local(i):
        if i == 0:
            return pltpu.make_async_copy(wd_h, wdb.at[pl.ds(0, fb)], w_l.at[i])
        return pltpu.make_async_copy((wg_h, wu_h)[i - 1], wgu.at[:, pl.ds((i - 1) * 2 * fb, fb)], w_l.at[i])

    def w_remote(i, k):
        if i == 0:
            src, dst = wd_h.at[pl.ds(k * fh, fh)], wdb.at[pl.ds(fb + k * fh, fh)]
        else:
            src = (wg_h, wu_h)[i - 1].at[:, pl.ds(k * fh, fh)]
            dst = wgu.at[:, pl.ds((i - 1) * 2 * fb + fb + k * fh, fh)]
        return remote(src, dst, w_s.at[i, k], w_r.at[i, k], mates[k][0])

    def swap(i, k):
        if i == 0:
            src, dst = accd.at[pl.ds(fb + k * fh, fh)], rec_d.at[pl.ds(k * fh, fh)]
        else:
            src = accw.at[:, pl.ds((i - 1) * 2 * fb + fb + k * fh, fh)]
            dst = (rec_g, rec_u)[i - 1].at[:, pl.ds(k * fh, fh)]
        return remote(src, dst, e_s.at[i, k], e_r.at[i, k], mates[k][0])

    def own_out(i):
        if i == 0:
            return pltpu.make_async_copy(accd.at[pl.ds(0, fb)], dwd_h, o_l.at[0])
        return pltpu.make_async_copy(accw.at[:, pl.ds((i - 1) * 2 * fb, fb)], (dwg_h, own_u)[i - 1], o_l.at[i])

    def rs_hop(j, d, z):
        a, b = lax.rem(j, 2), lax.rem(j + 1, S)
        return remote(rso.at[a, d, z], rsb.at[b, d, z], rs_s.at[a, d, z], rs_r.at[b, d, z], down[d])

    def part_hop(j):
        a, b = lax.rem(j, 2), lax.rem(j, S)
        return remote(sout.at[a], sin.at[b], p_s.at[a], p_r.at[b], sib)

    barrier = pltpu.get_barrier_semaphore()
    for dev in down + [sib, mates[0][0], mates[1][0]]:
        pl.semaphore_signal(barrier, inc=1, device_id={"tp": dev}, device_id_type=MESH)
    for i in range(3):
        w_local(i).start()
    pl.semaphore_wait(barrier, 5)
    for d in range(2):
        ring(0, 0, d, True).start()
        away(0, d, True).start()
    for d in range(2):
        ring(1, 0, d, True).start()
        cross(0, 0, d, True).start()
        cross(1, 0, d, True).start()

    def zero(i, _):
        accd[pl.ds(pl.multiple_of(i * (2 * fb // 8), 2 * fb // 8), 2 * fb // 8), :] = jnp.zeros((2 * fb // 8, h), F32)
        accw[pl.ds(pl.multiple_of(i * (h // 8), h // 8), h // 8), :] = jnp.zeros((h // 8, 4 * fb), F32)
        return 0

    lax.fori_loop(0, 8, zero, 0)

    ct = min(512, h)
    ht = min(256, h)

    def pass_dy(s):
        for d in range(2):
            ring(0, s - 1, d).wait_recv()

            @pl.when(s < m - 1)
            def _(d=d):
                ring(0, s, d).start()

            cross(0, s, d).start()

    def each_piece(k, do):
        for kk in range(side - 1):
            @pl.when(k == kk)
            def _(kk=kk):
                for d in range(2):
                    do(kk, d)

    def relay_x(k):
        def do(kk, d):
            away(kk, d).wait_recv()
            relay(kk, d).start()

        each_piece(k, do)

    def pass_even_x(s):
        def arrived(kk, d):
            relay(kk, d).wait_recv()
            if near[kk] < hb:
                spill(kk, d).wait_recv()

        each_piece(s // 2 - 1, arrived)
        each_piece(s // 2, lambda kk, d: away(kk, d).start())
        for d in range(2):
            ring(1, s, d).start()
            cross(1, s, d).start()

    def take_odd_x(s):
        for d in range(2):
            ring(1, s - 1, d).wait_recv()

        def pass_rest(kk, d):
            if near[kk] < hb:
                spill(kk, d).start()

        each_piece(s // 2, pass_rest)
        for d in range(2):
            cross(1, s, d).start()

    def grads(t):
        b = lax.rem(t, 2)

        @pl.when(t == 0)
        def _():
            w_local(0).wait()
            for k in range(2):
                w_remote(0, k).wait_recv()

        for k in range(2):
            u_all(t, k).wait_recv()
        pltpu.make_async_copy(uo.at[b], uo.at[b], u_l.at[b]).wait()
        tile_wait(0, t)
        for f in range(2):
            gbuf[:, f * fb:(f + 1) * fb] = dot(dyt[b].reshape(2 * tb, h), wdb[f * fb:(f + 1) * fb, :], 1, 1)

        def act(r, _):
            c, d = r // 2, lax.rem(r, 2)
            rws = pl.ds(pl.multiple_of(r * hb, hb), hb)
            half = pl.ds(pl.multiple_of(d * hb, hb), hb)
            for lo, n, get in (
                (0, fb, lambda j: uo[b, j, c, d]),
                (fb, fh, lambda j: ux[t, 0, j, c, d]),
                (fb + fh, fh, lambda j: ux[t, 1, j, c, d]),
            ):
                g = gbuf[rws, lo:lo + n]
                ug = get(0).astype(F32)
                uu = get(1).astype(F32)
                sg = jax.nn.sigmoid(ug)
                a = ug * sg
                zb[rws, lo:lo + n] = (a * uu).astype(BF16)
                dub[t, c, half, lo:lo + n] = (g * uu * sg * (1.0 + ug * (1.0 - sg))).astype(BF16)
                dub[t, c, half, 2 * fb + lo:2 * fb + lo + n] = (g * a).astype(BF16)
            return 0

        lax.fori_loop(0, 4, act, 0)

        def dwd_tile(j, _):
            cols = pl.ds(pl.multiple_of(j * ct, ct), ct)
            accd[:, cols] += dot(zb[...], dyt[b, :, :, :, cols].reshape(2 * tb, ct), 0, 0)
            return 0

        lax.fori_loop(0, h // ct, dwd_tile, 0)

    def weight_grads(t):
        b = lax.rem(t, 2)

        tile_wait(1, t)

        def dw_tile(j, _):
            cols = pl.ds(pl.multiple_of(j * ht, ht), ht)
            accw[cols, :] += dot(xt[b, :, :, :, cols].reshape(2 * tb, ht), dub[t].reshape(2 * tb, 4 * fb), 0, 0)
            return 0

        lax.fori_loop(0, h // ht, dw_tile, 0)

    def partial(j):
        t = lax.rem(j, m)
        b = lax.rem(j, 2)

        @pl.when(j == 1)
        def _():
            for i in (1, 2):
                w_local(i).wait()
                for k in range(2):
                    w_remote(i, k).wait_recv()

        @pl.when(j >= 3)
        def _():
            part_hop(j - 2).wait_send()

        def send_tile(c, _):
            cols = pl.ds(pl.multiple_of(c * ct, ct), ct)
            sout[b, :, cols] = dot(dub[t, other], wgu[cols, :], 1, 1).astype(BF16)
            return 0

        lax.fori_loop(0, h // ct, send_tile, 0)

        def keep_tile(c, _):
            cols = pl.ds(pl.multiple_of(c * ct, ct), ct)
            pbuf[b, :, cols] = dot(dub[t, core], wgu[cols, :], 1, 1)
            return 0

        lax.fori_loop(0, h // ct, keep_tile, 0)
        part_hop(j).start()

    def total(j, d, z, first):
        lo = pl.multiple_of(d * hb + z * q4, q4)
        v = pbuf[lax.rem(j, 2), pl.ds(lo, q4), :] + sin[lax.rem(j, S), pl.ds(lo, q4), :].astype(F32)
        if not first:
            v = v + rsb[lax.rem(j, S), d, z].astype(F32)
        return v.astype(BF16)

    def pass_sum(i):
        j, z = i // 2, lax.rem(i, 2)

        @pl.when(z == 0)
        def _():
            part_hop(j).wait_recv()

        @pl.when(j >= 3)
        def _():
            for d in range(2):
                rs_hop(j - 2, d, z).wait_send()

        @pl.when(j >= 2)
        def _():
            for d in range(2):
                rs_hop(j - 1, d, z).wait_recv()
                rso[lax.rem(j, 2), d, z] = total(j, d, z, False)

        @pl.when(j == 1)
        def _():
            for d in range(2):
                rso[lax.rem(j, 2), d, z] = total(j, d, z, True)

        for d in range(2):
            rs_hop(j, d, z).start()

    def swaps(i):
        for which in ((0,), (1, 2)):
            @pl.when(i == which[0])
            def _(which=which):
                for w in which:
                    for k in range(2):
                        swap(w, k).start()
                    if w == 2:
                        own_out(w).start()

    def fold(i):
        @pl.when(i == 0)
        def _():
            for k in range(2):
                swap(0, k).wait_recv()
            accd[0:fb, :] += rec_d[...]
            own_out(0).start()

        @pl.when(i == 1)
        def _():
            for k in range(2):
                swap(1, k).wait_recv()
            accw[:, 0:fb] += rec_g[...]
            own_out(1).start()

    def send_weight(i):
        for w in range(3):
            @pl.when(i == w)
            def _(w=w):
                for k in range(2):
                    w_remote(w, k).start()

    work = dict(
        Y=pass_dy, L=relay_x, E=pass_even_x, O=take_odd_x, a=lambda t: tile_load(0, t), c=lambda t: tile_load(1, t),
        A=grads, C=weight_grads, P=partial, R=pass_sum, S=swaps, D=fold, U=u_send, W=send_weight,
    )
    packed = [KINDS.index(w[0]) * 16 + int(w[1:]) for w in PLAN]

    def step(i, _):
        op = jnp.int32(packed[0])
        for k, code in enumerate(packed[1:], 1):
            op = jnp.where(i == k, code, op)
        kind, arg = op // 16, lax.rem(op, 16)
        for k, name in enumerate(KINDS):
            @pl.when(kind == k)
            def _(name=name):
                work[name](arg)
        return 0

    lax.fori_loop(0, len(packed), step, 0)

    part_hop(m).wait_recv()
    outs = []
    for d in range(2):
        for z in range(2):
            rs_hop(m - 2, d, z).wait_send()
    for z in range(2):
        for d in range(2):
            rs_hop(m - 1, d, z).wait_recv()
            rso[m % 2, d, z] = total(m, d, z, False)
            outs.append(pltpu.make_async_copy(rso.at[m % 2, d, z], dx_h.at[pl.ds(d * hb + z * q4, q4)], o_l.at[3 + 2 * d + z]))
            outs[-1].start()

    for i in range(3):
        own_out(i).wait()
        for k in range(2):
            swap(i, k).wait_send()
            if i == 2:
                swap(i, k).wait_recv()
            w_remote(i, k).wait_send()
    for j in (m - 1, m):
        part_hop(j).wait_send()
    for d in range(2):
        for z in range(2):
            rs_hop(m - 1, d, z).wait_send()

    def drain(s, _):
        for k in range(2):
            u_all(s, k).wait_send()
        for i in range(2):
            for d in range(2):
                cross(i, s, d).wait_send()

                @pl.when(s < m - 1 if i == 0 else lax.rem(s, 2) == 0)
                def _(i=i, d=d):
                    ring(i, s, d).wait_send()
        return 0

    lax.fori_loop(0, m, drain, 0)
    for k in range(side - 1):
        for d in range(2):
            away(k, d).wait_send()
            relay(k, d).wait_send()
            if near[k] < hb:
                spill(k, d).wait_send()
    for c in outs:
        c.wait()


def finish(dx, dwd, dwg, own_u, rec_u, dx_o, d_o, g_o, u_o):
    dx_o[...] = dx[...]
    d_o[...] = dwd[...]
    g_o[...] = dwg[...]
    u_o[...] = own_u[...] + rec_u[...]


def solution(mesh):
    tok = P(("dp", "tp"), None)
    col = P(None, "tp")
    row = P("tp", None)
    act = P("dp", "tp")
    n = mesh.shape["tp"] // 2
    side = math.isqrt(n)
    m = 2 * side

    def body(x, dy, wg, wu, wd, ug, uu):
        tb, h = x.shape
        fb = wg.shape[1]
        hb, fh = tb // 2, fb // 2
        vm = pltpu.VMEM
        dma = pltpu.SemaphoreType.DMA
        sds = jax.ShapeDtypeStruct
        flops = 12 * n * tb * h * 2 * fb
        dx, dwd, dwg, own_u, rec_u, _, _, _ = pl.pallas_call(
            functools.partial(kernel, side),
            out_shape=(
                sds((tb, h), BF16),
                sds((fb, h), F32), sds((h, fb), F32), sds((h, fb), F32), sds((h, fb), F32),
                sds((m, 2, 2, hb, h), BF16), sds((m, 2, 2, hb, h), BF16), sds((side - 1, 2, hb, h), BF16),
            ),
            in_specs=[pl.BlockSpec(memory_space=pltpu.HBM)] * 7,
            out_specs=[pl.BlockSpec(memory_space=pl.ANY)] * 8,
            scratch_shapes=[
                vm((2, 2, 2, hb, h), BF16),
                vm((2, 2, 2, hb, h), BF16),
                vm((2, 2, 2, 2, hb, fb), BF16),
                vm((m, 2, 2, 2, 2, hb, fh), BF16),
                vm((2 * fb, h), BF16),
                vm((h, 4 * fb), BF16),
                vm((2 * tb, 2 * fb), F32),
                vm((2 * tb, 2 * fb), BF16),
                vm((m, 2, tb, 4 * fb), BF16),
                vm((2 * fb, h), F32),
                vm((h, 4 * fb), F32),
                vm((2, tb, h), F32),
                vm((S, tb, h), BF16),
                vm((2, tb, h), BF16),
                vm((S, 2, 2, hb // 2, h), BF16),
                vm((2, 2, 2, hb // 2, h), BF16),
                vm((fb, h), F32),
                vm((h, fb), F32),
                dma((m, 2)), dma((m, 2)), dma((m, 2)), dma((m, 2)),
                dma((m, 2)), dma((m, 2)), dma((m, 2)), dma((m, 2)),
                dma((2,)), dma((2,)), dma((m, 2)), dma((m, 2)), dma((2,)),
                dma((3, 2)), dma((3, 2)), dma((3,)), dma((2,)), dma((S,)),
                dma((2, 2, 2)), dma((S, 2, 2)), dma((3, 2)), dma((3, 2)), dma((7,)),
                dma((side - 1, 2)), dma((side - 1, 2)), dma((side - 1, 2)), dma((side - 1, 2)),
            ],
            compiler_params=pltpu.CompilerParams(
                collective_id=0, has_side_effects=True, vmem_limit_bytes=62 * 1024 * 1024
            ),
            cost_estimate=pl.CostEstimate(flops=flops, bytes_accessed=2 * flops // 1000, transcendentals=0),
        )(
            x.reshape(2, hb, h), dy.reshape(2, hb, h), wg, wu, wd,
            ug.reshape(n, 2, 2, hb, fb), uu.reshape(n, 2, 2, hb, fb),
        )
        grid = 4

        def spec(r, c):
            return pl.BlockSpec((r // grid, c), lambda i: (i, 0))

        dx, dwd, dwg, dwu = pl.pallas_call(
            finish,
            grid=(grid,),
            out_shape=(sds((tb, h), BF16), sds((fb, h), F32), sds((h, fb), F32), sds((h, fb), F32)),
            in_specs=[spec(tb, h), spec(fb, h)] + [spec(h, fb)] * 3,
            out_specs=[spec(tb, h), spec(fb, h), spec(h, fb), spec(h, fb)],
        )(dx, dwd, dwg, own_u, rec_u)
        return dx, dwg, dwu, dwd

    return jax.shard_map(
        body, mesh=mesh, in_specs=(tok, tok, col, col, row, act, act), out_specs=(tok, act, act, tok), check_vma=False
    )
```

```python
import functools
import math

import jax
import jax.numpy as jnp
from jax import lax
from jax.experimental import pallas as pl
from jax.experimental.pallas import tpu as pltpu
from jax.sharding import PartitionSpec as P

F32 = jnp.float32
BF16 = jnp.bfloat16
S = 4
MESH = pl.DeviceIdType.MESH
SPLIT = (7, 6, 8)
PLAN = (
    "U1", "U0", "c0", "W0", "L0", "Y1", "a0", "O1", "Y2", "W2", "W1", "a1", "E2", "A0", "a2", "C0", "Y3",
    "c1", "U2", "U4", "A1", "U3", "O3", "U5", "C1", "P1", "Y4", "R2", "A2", "a3", "Y5", "c2", "P2", "L1",
    "R3", "U6", "A3", "P3", "a4", "Y6", "E4", "C2", "R4", "a5", "c3", "c4", "A4", "U7", "A5", "a6", "Y7",
    "L2", "R5", "C3", "A6", "a7", "P4", "O5", "A7", "E6", "c5", "S0", "C4", "R6", "R7", "c6", "C5", "C6",
    "O7", "c7", "C7", "R8", "S1", "R9", "P5", "P6", "R10", "R11", "R12", "P7", "D0", "D1", "R13", "R14", "P8",
    "R15",
)
KINDS = "YLEOacACPRSDUW"


def dot(a, b, ca, cb):
    return lax.dot_general(a, b, (((ca,), (cb,)), ((), ())), preferred_element_type=F32)


def kernel(
    side,
    x_h, dy_h, wg_h, wu_h, wd_h, ug_h, uu_h,
    dx_h, dwd_h, dwg_h, own_u, rec_u, dyl, xl, rl,
    dyt, xt, uo, ux, wdb, wgu, gbuf, zb, dub, accd, accw, pbuf, sin, sout, rsb, rso, rec_d, rec_g,
    dyr_s, dyr_r, dyc_s, dyc_r, xr_s, xr_r, xc_s, xc_r, dyt_l, xt_l, u_s, u_r, u_l,
    w_s, w_r, w_l, p_s, p_r, rs_s, rs_r, e_s, e_r, o_l, b_s, b_r, l_s, z_r,
):
    _, hb, h = dy_h.shape
    tb = 2 * hb
    q4 = hb // 2
    fb = wg_h.shape[1]
    fh = fb // 2
    m = 2 * side
    me = lax.axis_index("tp")
    chip = me // 2
    core = lax.rem(me, 2)
    other = 1 - core
    py = chip // side
    px = lax.rem(chip, side)
    cls = lax.rem(px + py, side)
    grp = cls // 2
    odd = lax.rem(cls, 2)

    def ring_pos(y, odd_):
        return 2 * lax.rem(side - y, side) + odd_

    def chip_at(g, i):
        k = i // 2
        return lax.rem(side - k, side) * side + lax.rem(k + lax.rem(i, 2) + 2 * g, side)

    def origin(g, pos, d, t):
        return chip_at(g, lax.rem(pos + (2 * m - t if d == 0 else t), m))

    pos = ring_pos(py, odd)
    down = [chip_at(grp, lax.rem(pos + 1, m)) * 2 + core, chip_at(grp, lax.rem(pos + m - 1, m)) * 2 + core]
    sib = chip * 2 + other
    step_ = side - 1 + 2 * odd
    mates = []
    for y, x in ((py, lax.rem(px + step_, side)), (lax.rem(py + step_, side), px)):
        c = lax.rem(x + y, side)
        mates.append(((y * side + x) * 2 + core, c // 2, ring_pos(y, lax.rem(c, 2))))

    leave = [jnp.where(odd == d, mates[1][0], mates[0][0]) for d in range(2)]

    def remote(src, dst, ss, rs, dev):
        return pltpu.make_async_remote_copy(
            src_ref=src, dst_ref=dst, send_sem=ss, recv_sem=rs, device_id={"tp": dev}, device_id_type=MESH
        )

    rows = ((dy_h, dyl, dyr_s, dyr_r, dyc_s, dyc_r, dyt, dyt_l), (x_h, xl, xr_s, xr_r, xc_s, xc_r, xt, xt_l))

    def ring(i, s, d, first=False):
        src, land, ss, rs = rows[i][:4]
        return remote(src.at[d] if first else land.at[s, core, d], land.at[s + 1, core, d], ss.at[s, d], rs.at[s + 1, d], down[d])

    near = [e * hb // 8 for e in SPLIT]

    def spill(k, d):
        s, rws = 2 * k + 1, pl.ds(near[k], hb - near[k])
        return remote(xl.at[s, core, d, rws], xl.at[s + 1, core, d, rws], xr_s.at[s, d], z_r.at[k, d], down[d])

    def away(k, d, first=False):
        rws = pl.ds(0, near[k])
        src = x_h.at[d, rws] if first else xl.at[2 * k, core, d, rws]
        return remote(src, rl.at[k, d, rws], b_s.at[k, d], b_r.at[k, d], leave[d])

    def relay(k, d):
        rws = pl.ds(0, near[k])
        return remote(rl.at[k, d, rws], xl.at[2 * k + 2, core, d, rws], l_s.at[k, d], xr_r.at[2 * k + 2, d], leave[d])

    def cross(i, s, d, first=False):
        src, land, ss, rs = rows[i][0], rows[i][1], rows[i][4], rows[i][5]
        return remote(src.at[d] if first else land.at[s, core, d], land.at[s, core, d], ss.at[s, d], rs.at[s, d], sib)

    def cross_in(i, s, d):
        land, ss, rs = rows[i][1], rows[i][4], rows[i][5]
        return remote(land.at[s, other, d], land.at[s, other, d], ss.at[s, d], rs.at[s, d], sib)

    def tile_wait(i, t):
        tile, sem = rows[i][6], rows[i][7]
        b = lax.rem(t, 2)
        pltpu.make_async_copy(tile.at[b], tile.at[b], sem.at[b]).wait()

    def tile_load(i, t):
        src, land, tile, sem = rows[i][0], rows[i][1], rows[i][6], rows[i][7]
        b = lax.rem(t, 2)
        for d in range(2):
            cross_in(i, t, d).wait_recv()

        @pl.when(t == 0)
        def _():
            pltpu.make_async_copy(src, tile.at[b, core], sem.at[b]).start()
            pltpu.make_async_copy(land.at[t, other], tile.at[b, other], sem.at[b]).start()

        @pl.when(t > 0)
        def _():
            pltpu.make_async_copy(land.at[t], tile.at[b], sem.at[b]).start()

        if i == 0:
            for d in range(2):
                o = origin(grp, pos, d, t)
                for j, u in enumerate((ug_h, uu_h)):
                    pltpu.make_async_copy(u.at[o, :, d], uo.at[b, j, :, d], u_l.at[b]).start()

    def u_send(t):
        for k, (dev, g, p) in enumerate(mates):
            for d in range(2):
                o = origin(g, p, d, t)
                for j, u in enumerate((ug_h, uu_h)):
                    remote(u.at[o, :, d, :, pl.ds(k * fh, fh)], ux.at[t, k, j, :, d], u_s.at[t, k], u_r.at[t, k], dev).start()

    def u_all(t, k):
        return remote(ux.at[t, k], ux.at[t, k], u_s.at[t, k], u_r.at[t, k], mates[k][0])

    def w_local(i):
        if i == 0:
            return pltpu.make_async_copy(wd_h, wdb.at[pl.ds(0, fb)], w_l.at[i])
        return pltpu.make_async_copy((wg_h, wu_h)[i - 1], wgu.at[:, pl.ds((i - 1) * 2 * fb, fb)], w_l.at[i])

    def w_remote(i, k):
        if i == 0:
            src, dst = wd_h.at[pl.ds(k * fh, fh)], wdb.at[pl.ds(fb + k * fh, fh)]
        else:
            src = (wg_h, wu_h)[i - 1].at[:, pl.ds(k * fh, fh)]
            dst = wgu.at[:, pl.ds((i - 1) * 2 * fb + fb + k * fh, fh)]
        return remote(src, dst, w_s.at[i, k], w_r.at[i, k], mates[k][0])

    def swap(i, k):
        if i == 0:
            src, dst = accd.at[pl.ds(fb + k * fh, fh)], rec_d.at[pl.ds(k * fh, fh)]
        else:
            src = accw.at[:, pl.ds((i - 1) * 2 * fb + fb + k * fh, fh)]
            dst = (rec_g, rec_u)[i - 1].at[:, pl.ds(k * fh, fh)]
        return remote(src, dst, e_s.at[i, k], e_r.at[i, k], mates[k][0])

    def own_out(i):
        if i == 0:
            return pltpu.make_async_copy(accd.at[pl.ds(0, fb)], dwd_h, o_l.at[0])
        return pltpu.make_async_copy(accw.at[:, pl.ds((i - 1) * 2 * fb, fb)], (dwg_h, own_u)[i - 1], o_l.at[i])

    def rs_hop(j, d, z):
        a, b = lax.rem(j, 2), lax.rem(j + 1, S)
        return remote(rso.at[a, d, z], rsb.at[b, d, z], rs_s.at[a, d, z], rs_r.at[b, d, z], down[d])

    def part_hop(j):
        a, b = lax.rem(j, 2), lax.rem(j, S)
        return remote(sout.at[a], sin.at[b], p_s.at[a], p_r.at[b], sib)

    barrier = pltpu.get_barrier_semaphore()
    for dev in down + [sib, mates[0][0], mates[1][0]]:
        pl.semaphore_signal(barrier, inc=1, device_id={"tp": dev}, device_id_type=MESH)
    for i in range(3):
        w_local(i).start()
    pl.semaphore_wait(barrier, 5)
    for d in range(2):
        ring(0, 0, d, True).start()
        away(0, d, True).start()
    for d in range(2):
        ring(1, 0, d, True).start()
        cross(0, 0, d, True).start()
        cross(1, 0, d, True).start()

    def zero(i, _):
        accd[pl.ds(pl.multiple_of(i * (2 * fb // 8), 2 * fb // 8), 2 * fb // 8), :] = jnp.zeros((2 * fb // 8, h), F32)
        accw[pl.ds(pl.multiple_of(i * (h // 8), h // 8), h // 8), :] = jnp.zeros((h // 8, 4 * fb), F32)
        return 0

    lax.fori_loop(0, 8, zero, 0)

    ct = min(512, h)
    ht = min(256, h)

    def pass_dy(s):
        for d in range(2):
            ring(0, s - 1, d).wait_recv()

            @pl.when(s < m - 1)
            def _(d=d):
                ring(0, s, d).start()

            cross(0, s, d).start()

    def each_piece(k, do):
        for kk in range(side - 1):
            @pl.when(k == kk)
            def _(kk=kk):
                for d in range(2):
                    do(kk, d)

    def relay_x(k):
        def do(kk, d):
            away(kk, d).wait_recv()
            relay(kk, d).start()

        each_piece(k, do)

    def pass_even_x(s):
        def arrived(kk, d):
            relay(kk, d).wait_recv()
            if near[kk] < hb:
                spill(kk, d).wait_recv()

        each_piece(s // 2 - 1, arrived)
        each_piece(s // 2, lambda kk, d: away(kk, d).start())
        for d in range(2):
            ring(1, s, d).start()
            cross(1, s, d).start()

    def take_odd_x(s):
        for d in range(2):
            ring(1, s - 1, d).wait_recv()

        def pass_rest(kk, d):
            if near[kk] < hb:
                spill(kk, d).start()

        each_piece(s // 2, pass_rest)
        for d in range(2):
            cross(1, s, d).start()

    def grads(t):
        b = lax.rem(t, 2)

        @pl.when(t == 0)
        def _():
            w_local(0).wait()
            for k in range(2):
                w_remote(0, k).wait_recv()

        for k in range(2):
            u_all(t, k).wait_recv()
        pltpu.make_async_copy(uo.at[b], uo.at[b], u_l.at[b]).wait()
        tile_wait(0, t)
        for f in range(2):
            gbuf[:, f * fb:(f + 1) * fb] = dot(dyt[b].reshape(2 * tb, h), wdb[f * fb:(f + 1) * fb, :], 1, 1)

        def act(r, _):
            c, d = r // 2, lax.rem(r, 2)
            rws = pl.ds(pl.multiple_of(r * hb, hb), hb)
            half = pl.ds(pl.multiple_of(d * hb, hb), hb)
            for lo, n, get in (
                (0, fb, lambda j: uo[b, j, c, d]),
                (fb, fh, lambda j: ux[t, 0, j, c, d]),
                (fb + fh, fh, lambda j: ux[t, 1, j, c, d]),
            ):
                g = gbuf[rws, lo:lo + n]
                ug = get(0).astype(F32)
                uu = get(1).astype(F32)
                sg = jax.nn.sigmoid(ug)
                a = ug * sg
                zb[rws, lo:lo + n] = (a * uu).astype(BF16)
                dub[t, c, half, lo:lo + n] = (g * uu * sg * (1.0 + ug * (1.0 - sg))).astype(BF16)
                dub[t, c, half, 2 * fb + lo:2 * fb + lo + n] = (g * a).astype(BF16)
            return 0

        lax.fori_loop(0, 4, act, 0)

        def dwd_tile(j, _):
            cols = pl.ds(pl.multiple_of(j * ct, ct), ct)
            accd[:, cols] += dot(zb[...], dyt[b, :, :, :, cols].reshape(2 * tb, ct), 0, 0)
            return 0

        lax.fori_loop(0, h // ct, dwd_tile, 0)

    def weight_grads(t):
        b = lax.rem(t, 2)

        tile_wait(1, t)

        def dw_tile(j, _):
            cols = pl.ds(pl.multiple_of(j * ht, ht), ht)
            accw[cols, :] += dot(xt[b, :, :, :, cols].reshape(2 * tb, ht), dub[t].reshape(2 * tb, 4 * fb), 0, 0)
            return 0

        lax.fori_loop(0, h // ht, dw_tile, 0)

    def partial(j):
        t = lax.rem(j, m)
        b = lax.rem(j, 2)

        @pl.when(j == 1)
        def _():
            for i in (1, 2):
                w_local(i).wait()
                for k in range(2):
                    w_remote(i, k).wait_recv()

        @pl.when(j >= 3)
        def _():
            part_hop(j - 2).wait_send()

        def send_tile(c, _):
            cols = pl.ds(pl.multiple_of(c * ct, ct), ct)
            sout[b, :, cols] = dot(dub[t, other], wgu[cols, :], 1, 1).astype(BF16)
            return 0

        lax.fori_loop(0, h // ct, send_tile, 0)

        def keep_tile(c, _):
            cols = pl.ds(pl.multiple_of(c * ct, ct), ct)
            pbuf[b, :, cols] = dot(dub[t, core], wgu[cols, :], 1, 1)
            return 0

        lax.fori_loop(0, h // ct, keep_tile, 0)
        part_hop(j).start()

    def total(j, d, z, first):
        lo = pl.multiple_of(d * hb + z * q4, q4)
        v = pbuf[lax.rem(j, 2), pl.ds(lo, q4), :] + sin[lax.rem(j, S), pl.ds(lo, q4), :].astype(F32)
        if not first:
            v = v + rsb[lax.rem(j, S), d, z].astype(F32)
        return v.astype(BF16)

    def pass_sum(i):
        j, z = i // 2, lax.rem(i, 2)

        @pl.when(z == 0)
        def _():
            part_hop(j).wait_recv()

        @pl.when(j >= 3)
        def _():
            for d in range(2):
                rs_hop(j - 2, d, z).wait_send()

        @pl.when(j >= 2)
        def _():
            for d in range(2):
                rs_hop(j - 1, d, z).wait_recv()
                rso[lax.rem(j, 2), d, z] = total(j, d, z, False)

        @pl.when(j == 1)
        def _():
            for d in range(2):
                rso[lax.rem(j, 2), d, z] = total(j, d, z, True)

        for d in range(2):
            rs_hop(j, d, z).start()

    def swaps(i):
        for which in ((0,), (1, 2)):
            @pl.when(i == which[0])
            def _(which=which):
                for w in which:
                    for k in range(2):
                        swap(w, k).start()
                    if w == 2:
                        own_out(w).start()

    def fold(i):
        @pl.when(i == 0)
        def _():
            for k in range(2):
                swap(0, k).wait_recv()
            accd[0:fb, :] += rec_d[...]
            own_out(0).start()

        @pl.when(i == 1)
        def _():
            for k in range(2):
                swap(1, k).wait_recv()
            accw[:, 0:fb] += rec_g[...]
            own_out(1).start()

    def send_weight(i):
        for w in range(3):
            @pl.when(i == w)
            def _(w=w):
                for k in range(2):
                    w_remote(w, k).start()

    work = dict(
        Y=pass_dy, L=relay_x, E=pass_even_x, O=take_odd_x, a=lambda t: tile_load(0, t), c=lambda t: tile_load(1, t),
        A=grads, C=weight_grads, P=partial, R=pass_sum, S=swaps, D=fold, U=u_send, W=send_weight,
    )
    packed = [KINDS.index(w[0]) * 16 + int(w[1:]) for w in PLAN]

    def step(i, _):
        op = jnp.int32(packed[0])
        for k, code in enumerate(packed[1:], 1):
            op = jnp.where(i == k, code, op)
        kind, arg = op // 16, lax.rem(op, 16)
        for k, name in enumerate(KINDS):
            @pl.when(kind == k)
            def _(name=name):
                work[name](arg)
        return 0

    lax.fori_loop(0, len(packed), step, 0)

    part_hop(m).wait_recv()
    outs = []
    for d in range(2):
        for z in range(2):
            rs_hop(m - 2, d, z).wait_send()
    for z in range(2):
        for d in range(2):
            rs_hop(m - 1, d, z).wait_recv()
            rso[m % 2, d, z] = total(m, d, z, False)
            outs.append(pltpu.make_async_copy(rso.at[m % 2, d, z], dx_h.at[pl.ds(d * hb + z * q4, q4)], o_l.at[3 + 2 * d + z]))
            outs[-1].start()

    for i in range(3):
        own_out(i).wait()
        for k in range(2):
            swap(i, k).wait_send()
            if i == 2:
                swap(i, k).wait_recv()
            w_remote(i, k).wait_send()
    for j in (m - 1, m):
        part_hop(j).wait_send()
    for d in range(2):
        for z in range(2):
            rs_hop(m - 1, d, z).wait_send()

    def drain(s, _):
        for k in range(2):
            u_all(s, k).wait_send()
        for i in range(2):
            for d in range(2):
                cross(i, s, d).wait_send()

                @pl.when(s < m - 1 if i == 0 else lax.rem(s, 2) == 0)
                def _(i=i, d=d):
                    ring(i, s, d).wait_send()
        return 0

    lax.fori_loop(0, m, drain, 0)
    for k in range(side - 1):
        for d in range(2):
            away(k, d).wait_send()
            relay(k, d).wait_send()
            if near[k] < hb:
                spill(k, d).wait_send()
    for c in outs:
        c.wait()


def finish(dx, dwd, dwg, own_u, rec_u, dx_o, d_o, g_o, u_o):
    dx_o[...] = dx[...]
    d_o[...] = dwd[...]
    g_o[...] = dwg[...]
    u_o[...] = own_u[...] + rec_u[...]


def solution(mesh):
    tok = P(("dp", "tp"), None)
    col = P(None, "tp")
    row = P("tp", None)
    act = P("dp", "tp")
    n = mesh.shape["tp"] // 2
    side = math.isqrt(n)
    m = 2 * side

    def body(x, dy, wg, wu, wd, ug, uu):
        tb, h = x.shape
        fb = wg.shape[1]
        hb, fh = tb // 2, fb // 2
        vm = pltpu.VMEM
        dma = pltpu.SemaphoreType.DMA
        sds = jax.ShapeDtypeStruct
        flops = 12 * n * tb * h * 2 * fb
        dx, dwd, dwg, own_u, rec_u, _, _, _ = pl.pallas_call(
            functools.partial(kernel, side),
            out_shape=(
                sds((tb, h), BF16),
                sds((fb, h), F32), sds((h, fb), F32), sds((h, fb), F32), sds((h, fb), F32),
                sds((m, 2, 2, hb, h), BF16), sds((m, 2, 2, hb, h), BF16), sds((side - 1, 2, hb, h), BF16),
            ),
            in_specs=[pl.BlockSpec(memory_space=pltpu.HBM)] * 7,
            out_specs=[pl.BlockSpec(memory_space=pl.ANY)] * 8,
            scratch_shapes=[
                vm((2, 2, 2, hb, h), BF16),
                vm((2, 2, 2, hb, h), BF16),
                vm((2, 2, 2, 2, hb, fb), BF16),
                vm((m, 2, 2, 2, 2, hb, fh), BF16),
                vm((2 * fb, h), BF16),
                vm((h, 4 * fb), BF16),
                vm((2 * tb, 2 * fb), F32),
                vm((2 * tb, 2 * fb), BF16),
                vm((m, 2, tb, 4 * fb), BF16),
                vm((2 * fb, h), F32),
                vm((h, 4 * fb), F32),
                vm((2, tb, h), F32),
                vm((S, tb, h), BF16),
                vm((2, tb, h), BF16),
                vm((S, 2, 2, hb // 2, h), BF16),
                vm((2, 2, 2, hb // 2, h), BF16),
                vm((fb, h), F32),
                vm((h, fb), F32),
                dma((m, 2)), dma((m, 2)), dma((m, 2)), dma((m, 2)),
                dma((m, 2)), dma((m, 2)), dma((m, 2)), dma((m, 2)),
                dma((2,)), dma((2,)), dma((m, 2)), dma((m, 2)), dma((2,)),
                dma((3, 2)), dma((3, 2)), dma((3,)), dma((2,)), dma((S,)),
                dma((2, 2, 2)), dma((S, 2, 2)), dma((3, 2)), dma((3, 2)), dma((7,)),
                dma((side - 1, 2)), dma((side - 1, 2)), dma((side - 1, 2)), dma((side - 1, 2)),
            ],
            compiler_params=pltpu.CompilerParams(
                collective_id=0, has_side_effects=True, vmem_limit_bytes=62 * 1024 * 1024
            ),
            cost_estimate=pl.CostEstimate(flops=flops, bytes_accessed=2 * flops // 1000, transcendentals=0),
        )(
            x.reshape(2, hb, h), dy.reshape(2, hb, h), wg, wu, wd,
            ug.reshape(n, 2, 2, hb, fb), uu.reshape(n, 2, 2, hb, fb),
        )
        grid = 4

        def spec(r, c):
            return pl.BlockSpec((r // grid, c), lambda i: (i, 0))

        dx, dwd, dwg, dwu = pl.pallas_call(
            finish,
            grid=(grid,),
            out_shape=(sds((tb, h), BF16), sds((fb, h), F32), sds((h, fb), F32), sds((h, fb), F32)),
            in_specs=[spec(tb, h), spec(fb, h)] + [spec(h, fb)] * 3,
            out_specs=[spec(tb, h), spec(fb, h), spec(h, fb), spec(h, fb)],
        )(dx, dwd, dwg, own_u, rec_u)
        return dx, dwg, dwu, dwd

    return jax.shard_map(
        body, mesh=mesh, in_specs=(tok, tok, col, col, row, act, act), out_specs=(tok, act, act, tok), check_vma=False
    )
```
